128 devices in a mesh: gx: 4 (over x_lo, core), gy: 8 (over x_hi, y), gz: 4 (over z).
Axes of the slice: x: 4 (x_hi: 2, x_lo: 2; x = x_hi * 2 + x_lo), y: 4, z: 4, core: 2. Of those that a mesh axis runs over, the one named last changes fastest.
Arguments:
- magnetization: float32 [3, 64, 256, 512], P(None, 'gx', 'gy', 'gz'), may hold values from -1 to 1, as said below
- kernel: float32 [6, 256, 512, 64], P(None, ('gx', 'gz'), 'gy'), may hold values from -3 to 3, as said below
- applied: float32 [3], replicated, may hold values from -4 to 4
Outputs:
- predicted: float32 [3, 64, 256, 512], P(None, 'gx', 'gy', 'gz')
- torque: float32 [3, 64, 256, 512], P(None, 'gx', 'gy', 'gz')
The draws below stay inside these ranges and needn't reach their ends.
Inputs may be any that keep to these rules, and one draw needn't show every extreme that they name: `magnetization`: each cell's three components form a vector of unit length. The tensor is even in wavenumber: kernel[c, ky, kz, kx] equals kernel[c, (256 - ky) mod 256, (512 - kz) mod 512, (64 - kx) mod 64].
All inputs are finite; a program needn't handle non-finite values.
Results may differ from the reference program's by a relative error of at most 0.00011.
Values sent between devices are 32-bit elements; how exact they have to be, the bound alone decides.
A program may use at most 128 MiB of HBM per device.

```python
import math
import jax
import jax.numpy as jnp
from jax import lax

NX = 64
NY = 256
NZ = 512


def draw_magnetization(key, part):
    key_one, key_two = jax.random.split(jax.random.fold_in(key, 11))
    extent = (NX, NY, NZ)
    height = jax.random.uniform(key_one, extent, jnp.float32, -1.0, 1.0)
    azimuth = jax.random.uniform(key_two, extent, jnp.float32, -math.pi, math.pi)
    radius = jnp.sqrt(jnp.maximum(1.0 - height * height, 0.0))
    return jnp.stack([radius * jnp.cos(azimuth), radius * jnp.sin(azimuth), height])


def draw_kernel(key, part):
    inner = jax.random.fold_in(key, 23)
    extent = (6, NY, NZ, NX)
    raw = jnp.clip(0.5 * jax.random.normal(inner, extent, jnp.float32), -3.0, 3.0)
    mirrored = jnp.roll(jnp.flip(raw, (1, 2, 3)), 1, (1, 2, 3))
    return 0.5 * (raw + mirrored)


def gaussian(own_key, dims, width, limit, held_as=jnp.bfloat16):
    entries = width * jax.random.normal(own_key, dims, jnp.float32)
    return jnp.clip(entries, min=-limit, max=limit).astype(held_as)


def setup_inputs(seed: int = 0) -> dict:
    streams_of = jax.random.split(jax.random.key(seed), 4)
    return {
        "magnetization": draw_magnetization(jax.random.fold_in(streams_of[3], 71), 0),
        "kernel": draw_kernel(jax.random.fold_in(streams_of[3], 71), 0),
        "applied": gaussian(streams_of[2], (3,), 1.0, 4.0, jnp.float32),
    }


exchange_coeff = 1.0
damping = 0.3
time_step = 0.2

def cross_product(first_vec, second_vec):
    return jnp.stack([first_vec[1] * second_vec[2] - first_vec[2] * second_vec[1], first_vec[2] * second_vec[0] - first_vec[0] * second_vec[2], first_vec[0] * second_vec[1] - first_vec[1] * second_vec[0]])

def reference(magnetization, kernel, applied):
    laplace = -6.0 * magnetization
    for dimension in (1, 2, 3):
        laplace = laplace + jnp.roll(magnetization, 1, dimension) + jnp.roll(magnetization, -1, dimension)
    spectrum = jnp.fft.fftn(magnetization, axes=(1, 2, 3))
    tensor = jnp.transpose(kernel, (0, 3, 1, 2))
    product_spectrum = jnp.stack([tensor[0] * spectrum[0] + tensor[3] * spectrum[1] + tensor[4] * spectrum[2], tensor[3] * spectrum[0] + tensor[1] * spectrum[1] + tensor[5] * spectrum[2], tensor[4] * spectrum[0] + tensor[5] * spectrum[1] + tensor[2] * spectrum[2]])
    demagnetizing = -jnp.real(jnp.fft.ifftn(product_spectrum, axes=(1, 2, 3)))
    total_field = demagnetizing + exchange_coeff * laplace + applied[:, None, None, None]
    precess = cross_product(magnetization, total_field)
    double_twist = cross_product(magnetization, precess)
    torque = -(precess + damping * double_twist) / (1.0 + damping * damping)
    stepped = magnetization + time_step * torque
    length = jnp.sqrt(lax.optimization_barrier(jnp.sum(stepped * stepped, axis=0)))
    return (stepped / length, torque)
```

```python
import math

import jax
import jax.numpy as jnp
import numpy as np
from jax import lax
from jax.experimental import pallas as pl
from jax.experimental.pallas import tpu as pltpu
from jax.sharding import PartitionSpec as P

MESH = pl.DeviceIdType.MESH
F32 = jnp.float32
BF16 = jnp.bfloat16
NX, NY, NZ = 64, 256, 512
EXCHANGE = 1.0
DAMPING = 0.3
STEP = 0.2
INVERSE_COUNT = 1.0 / (NX * NY * NZ)


def wave_z(block, slot):
    return 64 * block + slot + (block >= 4)


def turn(rows, cols, length):
    angle = 2.0 * np.pi / length * ((rows[:, None] * cols[None, :]) % length)
    return np.cos(angle), np.sin(angle)


def z_tables():
    block, part, slot = (a.reshape(-1) for a in np.meshgrid(np.arange(8), np.arange(2), np.arange(32), indexing="ij"))
    cosine, sine = turn(np.arange(NZ), wave_z(block, slot), NZ)
    forward = np.where(part == 0, cosine, -sine)
    alternate = 1.0 - 2.0 * (np.arange(NZ) % 2)
    packed = (block == 0) & (slot == 0)
    forward[:, packed & (part == 1)] = alternate[:, None]
    backward = np.where(packed, 1.0, 2.0)[:, None] * forward.T
    return forward, backward


def y_tables():
    part, group, owner, tile = (
        a.reshape(-1) for a in np.meshgrid(np.arange(2), np.arange(4), np.arange(16), np.arange(4), indexing="ij")
    )
    ky = 16 * owner + 4 * tile + group
    block, yp, row = (a.reshape(-1) for a in np.meshgrid(np.arange(8), np.arange(2), np.arange(32), indexing="ij"))
    y = 32 * block + row
    cosine, sine = turn(ky, y, NY)
    out_re, in_re = (part == 0)[:, None], (yp == 0)[None, :]
    forward = np.where(out_re == in_re, cosine, np.where(out_re, sine, -sine))
    backward = np.where(out_re == in_re, cosine, np.where(in_re, -sine, sine)).T
    low, high = ((ky > 0) & (ky < 128))[:, None], (ky > 128)[:, None]
    single = np.where(out_re, cosine, -sine)
    forward_packed = np.where(
        low, np.where(in_re, single, 0.0), np.where(high, np.where(in_re, 0.0, single), forward)
    )
    double = 2.0 * single
    backward_packed = np.where(
        low, np.where(in_re, double, 0.0), np.where(high, np.where(in_re, 0.0, double), backward.T)
    ).T
    return forward, forward_packed, backward, backward_packed


def x_tables():
    part, kx = (a.reshape(-1) for a in np.meshgrid(np.arange(2), np.arange(64), indexing="ij"))
    owner, xp, xs = (a.reshape(-1) for a in np.meshgrid(np.arange(16), np.arange(2), np.arange(4), indexing="ij"))
    cosine, sine = turn(kx, 4 * owner + xs, NX)
    out_re, in_re = (part == 0)[:, None], (xp == 0)[None, :]
    forward = np.where(out_re == in_re, cosine, np.where(out_re, sine, -sine))
    mirrored = np.where(in_re, forward, -forward)
    backward = np.where(out_re == in_re, cosine, np.where(in_re, -sine, sine)).T
    return forward, mirrored, backward


def eigen_tables():
    lam = lambda k, n: 2.0 * np.cos(2.0 * np.pi * k / n) - 2.0
    table = np.zeros((16, 8, 4, 128))
    for owner in range(16):
        for block in range(8):
            for tile in range(4):
                for group in range(4):
                    ky = 16 * owner + 4 * tile + group
                    kz = wave_z(block, np.arange(32))
                    row = lam(ky, NY) + lam(kz, NZ)
                    if block == 0:
                        row[0] = lam(ky, NY) + (-2.0 if ky % 128 == 0 else (-4.0 if ky > 128 else 0.0))
                    table[owner, block, tile, 32 * group : 32 * group + 32] = row
    return (
        (table * EXCHANGE).reshape(128, 4, 128).astype(np.float32),
        np.broadcast_to((lam(np.arange(64), NX) * EXCHANGE)[:, None], (64, 128)).astype(np.float32),
    )


def halves(table):
    table = np.asarray(table, np.float64)
    high = table.astype(np.float32).astype(jnp.bfloat16)
    low = (table - high.astype(np.float64)).astype(np.float32).astype(jnp.bfloat16)
    return np.stack([high, low])


def split(value):
    high = value.astype(BF16)
    return high, (value - high.astype(F32)).astype(BF16)


def dot(a, b):
    return jnp.dot(a, b, preferred_element_type=F32)


def right_product(value, table, index, cols):
    high, low = split(value)
    t_high, t_low = table[index, 0, :, cols], table[index, 1, :, cols]
    return dot(high, t_high) + dot(low, t_high) + dot(high, t_low)


def left_product(table, index, rows, high, low):
    t_high, t_low = table[index, 0, rows, :], table[index, 1, rows, :]
    return dot(t_high, high) + dot(t_high, low) + dot(t_low, high)


def swap_lanes(values):
    lane = lax.broadcasted_iota(jnp.int32, values[0].shape, 1)
    low_half = lane < 64
    even = (lane & 32) == 0
    v0, v1, v2, v3 = values
    roll = lambda v, s: pltpu.roll(v, s, 1)
    a0 = jnp.where(low_half, v0, roll(v2, 64))
    a2 = jnp.where(low_half, roll(v0, 64), v2)
    a1 = jnp.where(low_half, v1, roll(v3, 64))
    a3 = jnp.where(low_half, roll(v1, 64), v3)
    return (
        jnp.where(even, a0, roll(a1, 32)),
        jnp.where(even, roll(a0, 96), a1),
        jnp.where(even, a2, roll(a3, 32)),
        jnp.where(even, roll(a2, 96), a3),
    )


PAIR = ((0, 3, 4), (3, 1, 5), (4, 5, 2))
ZF, ZB, YF, YFP, YB, YBP = range(6)
XF, XM, XB = range(3)


def body(
    m_hbm, k_hbm, applied, tab_hbm, tabx_hbm, lam_hbm, lamx_hbm,
    pred_hbm, torque_hbm,
    m, kraw, tab, tabx, lam, lamx, kp, k2, kn_out, kn_in,
    r1, s2, r2, s3, r3, spec, s4, r4, s5, r5, s6, r6, pout, tout,
    local_sem, send_sem, recv_sem, kn_sems,
):
    gx, gy, gz = lax.axis_index("gx"), lax.axis_index("gy"), lax.axis_index("gz")
    ac = gx * 4 + gz
    loads = [
        pltpu.make_async_copy(m_hbm, m, local_sem.at[0]),
        pltpu.make_async_copy(tab_hbm, tab, local_sem.at[1]),
        pltpu.make_async_copy(k_hbm, kraw, local_sem.at[2]),
        pltpu.make_async_copy(tabx_hbm, tabx, local_sem.at[3]),
        pltpu.make_async_copy(lam_hbm.at[ac * 8 + gy], lam, local_sem.at[4]),
        pltpu.make_async_copy(lamx_hbm, lamx, local_sem.at[5]),
    ]
    for load in loads:
        load.start()

    by_z = lambda p: {"gz": p}
    by_y = lambda p: {"gy": p}
    by_xz = lambda p: {"gx": p // 4, "gz": lax.rem(p, 4)}

    barrier = pltpu.get_barrier_semaphore()

    def greet(count, me, place):
        def one(j, carry):
            pl.semaphore_signal(
                barrier, inc=1, device_id=place(lax.rem(me + j, count)), device_id_type=MESH
            )
            return carry

        lax.fori_loop(1, count, one, 0)

    greet(16, ac, by_xz)
    greet(8, gy, by_y)
    pl.semaphore_wait(barrier, 22)

    def copy(e, c, src, dst, device):
        return pltpu.make_async_remote_copy(
            src_ref=src, dst_ref=dst, send_sem=send_sem.at[e, c], recv_sem=recv_sem.at[e, c],
            device_id=device, device_id_type=MESH,
        )

    def send_all(e, c, src, dst, count, me, place):
        def one(j, carry):
            p = lax.rem(me + j, count)
            copy(e, c, src.at[c, p], dst.at[c, me], place(p)).start()
            return carry

        lax.fori_loop(1, count, one, 0)
        dst[c, me] = src[c, me]

    def arrived(e, c, dst, count):
        part = dst.at[c, pl.ds(0, count - 1)]
        copy(e, c, part, part, by_y(lax.rem(gy + 1, 8))).wait_recv()

    def each(step):
        def one(c, carry):
            step(c)
            return carry

        lax.fori_loop(0, 3, one, 0)

    loads[0].wait()
    each(lambda c: send_all(0, c, m, r1, 4, gz, by_z))

    loads[2].wait()

    @pl.when(gy == 4)
    def _():
        for cc in range(6):
            for i in range(16):
                kn_out[cc, i : i + 1, 0:64] = kraw[cc, i, 0:1, :]

    kn = pltpu.make_async_remote_copy(
        src_ref=kn_out, dst_ref=kn_in, send_sem=kn_sems.at[0], recv_sem=kn_sems.at[1],
        device_id=by_y(0), device_id_type=MESH,
    )

    @pl.when(gy == 4)
    def _():
        kn.start()

    for load in loads[1:2] + loads[3:]:
        load.wait()

    def z_forward(c):
        arrived(0, c, r1, 4)
        rows = jnp.concatenate([r1[c, s] for s in range(4)], axis=1)
        for h in range(2):
            out = right_product(rows, tab, ZF, pl.ds(256 * h, 256))
            for u in range(2):
                t = 2 * h + u
                parts = swap_lanes([out[32 * x : 32 * x + 32, 128 * u : 128 * u + 128] for x in range(4)])
                for q in range(4):
                    s2[c, 2 * t + q // 2, 32 * (q % 2) : 32 * (q % 2) + 32, :] = parts[q]
        send_all(1, c, s2, r2, 8, gy, by_y)

    each(z_forward)

    late = (gy >= 4).astype(jnp.int32)
    first = gy == 0

    @pl.when(first)
    def _():
        kn.wait_recv()

    far = first & (ac >= 8)
    middle = first & (lax.rem(ac, 8) == 0)

    def prepare(cc, carry):
        for v in range(4):
            blocks = []
            for g in range(4):
                i = 4 * v + g
                plain = kraw[cc, i, 0:32, :]
                shifted = kraw[cc, i, 1:33, :]
                block = jnp.where(late == 1, shifted, plain)
                row = lax.broadcasted_iota(jnp.int32, block.shape, 0)
                nyquist = jnp.broadcast_to(kn_in[cc, i : i + 1, 0:64], block.shape)
                nyquist = jnp.where(first, nyquist, block)
                if i == 0:
                    top = jnp.where(far, nyquist, block)
                    top = jnp.where(middle, 0.5 * (block + nyquist), top)
                    half = jnp.where(middle & (row == 0), 0.5 * (block - nyquist), 0.0)
                    half = jnp.concatenate([half, jnp.zeros((96, 64), F32)], axis=0)
                    k2[cc] = -INVERSE_COUNT * half.T
                else:
                    top = jnp.where(far, nyquist, block)
                blocks.append(jnp.where(row == 0, top, block))
            kp[cc, v] = -INVERSE_COUNT * jnp.concatenate(blocks, axis=0).T
        return carry

    lax.fori_loop(0, 6, prepare, 0)
    lane = lax.broadcasted_iota(jnp.int32, (64, 128), 1)
    corner = jnp.where(middle & (lane == 0), 2.0 * EXCHANGE * INVERSE_COUNT, 0.0)
    for cc in range(3):
        k2[cc] += corner
        for v in range(4):
            kp[cc, v] += INVERSE_COUNT * (lamx[...] + lam[v : v + 1, :])

    s3_blocks = s3.reshape(3, 16, 32, 128)
    r4_blocks = r4.reshape(3, 16, 32, 128)
    packed_lane = lambda shape: first & ((lax.broadcasted_iota(jnp.int32, shape, 1) & 31) == 0)

    def y_forward(c):
        arrived(1, c, r2, 8)
        high, low = split(r2[c].reshape(512, 128))
        for part in range(2):
            rows = pl.ds(256 * part, 256)
            out = left_product(tab, YF, rows, high, low)
            other = left_product(tab, YFP, rows, high, low)
            out = jnp.where(packed_lane(out.shape), other, out)
            parts = swap_lanes([out[64 * g : 64 * g + 64, :] for g in range(4)])
            for x in range(4):
                s3[c, pl.ds(4 * part + x, 64, stride=8), :] = parts[x]
        send_all(2, c, s3_blocks, r3, 16, ac, by_xz)

    each(y_forward)

    def x_forward(c):
        arrived(2, c, r3, 16)
        for v in range(4):
            high, low = split(r3[c, :, 8 * v : 8 * v + 8, :].reshape(128, 128))
            spec[c, v] = left_product(tabx, XF, pl.ds(0, 128), high, low)
            if v == 0:
                spec[c, 4] = left_product(tabx, XM, pl.ds(0, 128), high, low)

    each(x_forward)

    for c in range(3):
        for v in range(4):
            terms = []
            for part in range(2):
                rows = slice(64 * part, 64 * part + 64)
                total = sum(kp[PAIR[c][d], v] * spec[d, v, rows, :] for d in range(3))
                if v == 0:
                    total = total + sum(k2[PAIR[c][d]] * spec[d, 4, rows, :] for d in range(3))
                terms.append(total)
            high, low = split(jnp.concatenate(terms, axis=0))
            out = left_product(tabx, XB, pl.ds(0, 128), high, low)
            s4[c, :, 8 * v : 8 * v + 8, :] = out.reshape(16, 8, 128)
        send_all(3, c, s4, r4_blocks, 16, ac, by_xz)

    def y_backward(c):
        arrived(3, c, r4_blocks, 16)
        pieces = []
        for part in range(2):
            pieces += swap_lanes([r4[c, pl.ds(4 * part + x, 64, stride=8), :] for x in range(4)])
        high, low = split(jnp.concatenate(pieces, axis=0))
        for h in range(2):
            rows = pl.ds(256 * h, 256)
            out = left_product(tab, YB, rows, high, low)
            other = left_product(tab, YBP, rows, high, low)
            out = jnp.where(packed_lane(out.shape), other, out)
            s5[c, 4 * h : 4 * h + 4] = out.reshape(4, 64, 128)
        send_all(4, c, s5, r5, 8, gy, by_y)

    each(y_backward)

    def z_backward(c):
        arrived(4, c, r5, 8)
        tiles = []
        for t in range(4):
            parts = swap_lanes([r5[c, 2 * t + q // 2, 32 * (q % 2) : 32 * (q % 2) + 32, :] for q in range(4)])
            tiles.append(jnp.concatenate(parts, axis=0))
        rows = jnp.concatenate(tiles, axis=1)
        for h in range(2):
            out = right_product(rows, tab, ZB, pl.ds(256 * h, 256))
            s6[c, 2 * h] = out[:, 0:128]
            s6[c, 2 * h + 1] = out[:, 128:256]
        send_all(5, c, s6, r6, 4, gz, by_z)

    each(z_backward)
    each(lambda c: arrived(5, c, r6, 4))

    def finish(n, carry):
        s, piece = n // 4, lax.rem(n, 4)
        rows = pl.ds(32 * piece, 32)
        mag = [m[c, s, rows, :] for c in range(3)]
        field = [r6[c, s, rows, :] + applied[c] for c in range(3)]
        cross = lambda a, b: [
            a[1] * b[2] - a[2] * b[1],
            a[2] * b[0] - a[0] * b[2],
            a[0] * b[1] - a[1] * b[0],
        ]
        precess = cross(mag, field)
        twist = cross(mag, precess)
        torque = [-(precess[c] + DAMPING * twist[c]) / (1.0 + DAMPING * DAMPING) for c in range(3)]
        stepped = [mag[c] + STEP * torque[c] for c in range(3)]
        length = jnp.sqrt(stepped[0] * stepped[0] + stepped[1] * stepped[1] + stepped[2] * stepped[2])
        for c in range(3):
            tout[c, s, rows, :] = torque[c]
            pout[c, s, rows, :] = stepped[c] / length
        return carry

    lax.fori_loop(0, 16, finish, 0)
    stores = [
        pltpu.make_async_copy(pout, pred_hbm, local_sem.at[0]),
        pltpu.make_async_copy(tout, torque_hbm, local_sem.at[1]),
    ]
    for store in stores:
        store.start()

    def sent(e, src, count):
        def one(c, carry):
            part = src.at[c, pl.ds(0, count - 1)]
            copy(e, c, part, part, by_y(lax.rem(gy + 1, 8))).wait_send()
            return carry

        lax.fori_loop(0, 3, one, 0)

    sent(0, m, 4)
    sent(1, s2, 8)
    sent(2, s3_blocks, 16)
    sent(3, s4, 16)
    sent(4, s5, 8)
    sent(5, s6, 4)

    @pl.when(gy == 4)
    def _():
        kn.wait_send()

    for store in stores:
        store.wait()


def shards(magnetization, kernel, applied):
    tab = np.stack([halves(t) for t in (*z_tables(), *y_tables())])
    tabx = np.stack([halves(t) for t in x_tables()])
    lam, lamx = eigen_tables()
    block = (3, 4, 128, 128)
    anywhere = pl.BlockSpec(memory_space=pl.ANY)
    vmem = lambda *shape, dtype=F32: pltpu.VMEM(shape, dtype)
    predicted, torque = pl.pallas_call(
        body,
        out_shape=[jax.ShapeDtypeStruct(block, F32)] * 2,
        in_specs=[anywhere, anywhere, pl.BlockSpec(memory_space=pltpu.SMEM)] + [anywhere] * 4,
        out_specs=[anywhere] * 2,
        scratch_shapes=[
            vmem(*block),
            vmem(6, 16, 64, 64),
            vmem(6, 2, 512, 512, dtype=BF16),
            vmem(3, 2, 128, 128, dtype=BF16),
            vmem(4, 128),
            vmem(64, 128),
            vmem(6, 4, 64, 128),
            vmem(6, 64, 128),
            vmem(6, 16, 128),
            vmem(6, 16, 128),
            vmem(*block),
            vmem(3, 8, 64, 128),
            vmem(3, 8, 64, 128),
            vmem(3, 512, 128),
            vmem(3, 16, 32, 128),
            vmem(3, 5, 128, 128),
            vmem(3, 16, 32, 128),
            vmem(3, 512, 128),
            vmem(3, 8, 64, 128),
            vmem(3, 8, 64, 128),
            vmem(*block),
            vmem(*block),
            vmem(*block),
            vmem(*block),
            pltpu.SemaphoreType.DMA((6,)),
            pltpu.SemaphoreType.DMA((6, 3)),
            pltpu.SemaphoreType.DMA((6, 3)),
            pltpu.SemaphoreType.DMA((2,)),
        ],
        compiler_params=pltpu.CompilerParams(
            collective_id=0, has_side_effects=True, vmem_limit_bytes=56 * 1024 * 1024
        ),
    )(
        magnetization.reshape(block), kernel, applied,
        jnp.asarray(tab), jnp.asarray(tabx), jnp.asarray(lam), jnp.asarray(lamx),
    )
    shape = magnetization.shape
    return predicted.reshape(shape), torque.reshape(shape)


def solution(mesh):
    return jax.shard_map(
        shards,
        mesh=mesh,
        in_specs=(P(None, "gx", "gy", "gz"), P(None, ("gx", "gz"), "gy", None), P()),
        out_specs=(P(None, "gx", "gy", "gz"), P(None, "gx", "gy", "gz")),
        check_vma=False,
    )
```

```python
import math

import jax
import jax.numpy as jnp
import numpy as np
from jax import lax
from jax.experimental import pallas as pl
from jax.experimental.pallas import tpu as pltpu
from jax.sharding import PartitionSpec as P

MESH = pl.DeviceIdType.MESH
F32 = jnp.float32
BF16 = jnp.bfloat16
NX, NY, NZ = 64, 256, 512
EXCHANGE = 1.0
DAMPING = 0.3
STEP = 0.2
INVERSE_COUNT = 1.0 / (NX * NY * NZ)


def wave_z(block, slot):
    odd = slot >= 16
    return 64 * block + 2 * (slot % 16) + np.where(odd, 1, np.where(block >= 4, 2, 0))


def turn(rows, cols, length):
    angle = 2.0 * np.pi / length * ((rows[:, None] * cols[None, :]) % length)
    return np.cos(angle), np.sin(angle)


def grid(*counts):
    return [a.reshape(-1) for a in np.meshgrid(*(np.arange(n) for n in counts), indexing="ij")]


def z_tables():
    forward, backward = [], []
    for parity in range(2):
        block, part, slot = grid(8, 2, 16)
        cosine, sine = turn(np.arange(NZ // 2), wave_z(block, slot + 16 * parity), NZ)
        table = np.where(part == 0, cosine, -sine)
        weight = np.full(256, 2.0)
        if parity == 0:
            packed = (block == 0) & (slot == 0)
            alternate = 1.0 - 2.0 * (np.arange(NZ // 2) % 2)
            table[:, packed & (part == 1)] = alternate[:, None]
            weight[packed] = 1.0
        forward.append(table)
        backward.append(weight[:, None] * table.T)
    return forward, backward


def y_tables():
    forward, backward = [], []
    for parity in range(2):
        part, group, owner, tile = grid(2, 2, 16, 4)
        ky = 16 * owner + 4 * tile + 2 * group + parity
        half, block, yp, row = grid(2, 4, 2, 16)
        cosine, sine = turn(ky, 32 * block + 16 * half + row, NY)
        out_re, in_re = (part == 0)[:, None], (yp == 0)[None, :]
        plain = np.where(out_re == in_re, cosine, np.where(out_re, sine, -sine))
        low, high = ((ky > 0) & (ky < 128))[:, None], (ky > 128)[:, None]
        single = np.where(out_re, cosine, -sine)
        packed = np.where(low, np.where(in_re, single, 0.0), np.where(high, np.where(in_re, 0.0, single), plain))
        weight = np.where(low | high, 2.0, 1.0)
        forward.append(np.concatenate([plain, packed], axis=0))
        backward.append(np.concatenate([plain.T, (weight * packed).T], axis=0))
    return forward, backward


def x_tables():
    part, kx = grid(2, 64)
    owner, xp, xs = grid(16, 2, 4)
    cosine, sine = turn(kx, 4 * owner + xs, NX)
    out_re, in_re = (part == 0)[:, None], (xp == 0)[None, :]
    forward = np.where(out_re == in_re, cosine, np.where(out_re, sine, -sine))
    mirrored = np.where(in_re, forward, -forward)
    backward = np.where(out_re == in_re, cosine, np.where(in_re, -sine, sine)).T
    return forward, mirrored, backward


def eigen_tables():
    lam = lambda k, n: 2.0 * np.cos(2.0 * np.pi * k / n) - 2.0
    table = np.zeros((16, 8, 4, 128))
    for owner in range(16):
        for block in range(8):
            for tile in range(4):
                for group in range(4):
                    ky = 16 * owner + 4 * tile + group
                    kz = wave_z(block, np.arange(32))
                    row = lam(ky, NY) + lam(kz, NZ)
                    if block == 0:
                        row[0] = lam(ky, NY) + (-2.0 if ky % 128 == 0 else (-4.0 if ky > 128 else 0.0))
                    table[owner, block, tile, 32 * group : 32 * group + 32] = row
    return (
        (table * EXCHANGE).reshape(128, 4, 128).astype(np.float32),
        np.broadcast_to((lam(np.arange(64), NX) * EXCHANGE)[:, None], (64, 128)).astype(np.float32),
    )


def halves(table):
    table = np.asarray(table, np.float64)
    high = table.astype(np.float32).astype(jnp.bfloat16)
    low = (table - high.astype(np.float64)).astype(np.float32).astype(jnp.bfloat16)
    return np.stack([high, low])


def split(value):
    high = value.astype(BF16)
    return high, (value - high.astype(F32)).astype(BF16)


def dot(a, b):
    return jnp.dot(a, b, preferred_element_type=F32)


def right_product(value, table, index):
    high, low = split(value)
    rows = value.shape[0]
    both = dot(jnp.concatenate([high, low], axis=0), table[index, 0])
    return both[:rows] + both[rows:] + dot(high, table[index, 1])


def left_product(table, index, value):
    high, low = split(value)
    cols = value.shape[1]
    both = dot(table[index, 0], jnp.concatenate([high, low], axis=1))
    return both[:, :cols] + both[:, cols:] + dot(table[index, 1], high)


def swap_lanes(values):
    values = list(values)
    lane = lax.broadcasted_iota(jnp.int32, values[0].shape, 1)
    step = len(values) // 2
    width = 64
    while step:
        low = (lane & width) == 0
        for i in range(len(values)):
            if i & step == 0:
                a, b = values[i], values[i + step]
                values[i] = jnp.where(low, a, pltpu.roll(b, width, 1))
                values[i + step] = jnp.where(low, pltpu.roll(a, 128 - width, 1), b)
        step //= 2
        width //= 2
    return values


PAIR = ((0, 3, 4), (3, 1, 5), (4, 5, 2))
FORWARD, BACKWARD = 0, 2
XF, XM, XB = range(3)


def transform(
    m_hbm, k_hbm, tabz_hbm, taby_hbm, tabx_hbm, lam_hbm, lamx_hbm,
    m, r6,
    kraw, tabz, tabyf, tabyb, tabx, lam, lamx, kp, k2, kn_out, kn_in,
    r1, s2, r2, s3, r3, spec, s4, r4, s5, r5, s6,
    local_sem, send_sem, recv_sem, kn_sems,
):
    gx, gy, gz = lax.axis_index("gx"), lax.axis_index("gy"), lax.axis_index("gz")
    ac = gx * 4 + gz
    load_m = pltpu.make_async_copy(m_hbm, m, local_sem.at[0])
    load_m.start()

    by_z = lambda p: {"gz": p}
    by_y = lambda p: {"gy": p}
    by_xz = lambda p: {"gx": p // 4, "gz": lax.rem(p, 4)}

    barrier = pltpu.get_barrier_semaphore()

    def repeat(start, stop, step):
        def one(j, carry):
            step(j)
            return carry

        lax.fori_loop(start, stop, one, 0)

    def greet(count, me, place):
        repeat(
            1,
            count,
            lambda j: pl.semaphore_signal(
                barrier, inc=1, device_id=place(lax.rem(me + j, count)), device_id_type=MESH
            ),
        )

    greet(16, ac, by_xz)
    greet(8, gy, by_y)
    pl.semaphore_wait(barrier, 22)

    def copy(e, n, src, dst, device):
        return pltpu.make_async_remote_copy(
            src_ref=src, dst_ref=dst, send_sem=send_sem.at[e, n], recv_sem=recv_sem.at[e, n],
            device_id=device, device_id_type=MESH,
        )

    def send_all(e, n, src, dst, count, me, place):
        def one(j):
            p = lax.rem(me + j, count)
            copy(e, n, src.at[n, p], dst.at[n, me], place(p)).start()

        repeat(1, count, one)
        dst[n, me] = src[n, me]

    def arrived(e, n, dst, count):
        part = dst.at[n, pl.ds(0, count - 1)]
        copy(e, n, part, part, by_y(lax.rem(gy + 1, 8))).wait_recv()

    load_m.wait()
    m_blocks = m.reshape(3, 4, 4, 32, 128)

    def send_m(n):
        c, half = n // 2, lax.rem(n, 2)
        rows = pl.ds(pl.multiple_of(16 * half, 16), 16)

        def one(j):
            p = lax.rem(gz + j, 4)
            copy(0, n, m_blocks.at[c, p, :, rows, :], r1.at[n, gz], by_z(p)).start()

        repeat(1, 4, one)
        r1[n, gz] = m_blocks[c, gz, :, rows, :]

    repeat(0, 6, send_m)

    loads = [
        pltpu.make_async_copy(tabz_hbm, tabz, local_sem.at[0]),
        pltpu.make_async_copy(k_hbm, kraw, local_sem.at[1]),
        pltpu.make_async_copy(lam_hbm.at[ac * 8 + gy], lam, local_sem.at[2]),
        pltpu.make_async_copy(lamx_hbm, lamx, local_sem.at[3]),
        pltpu.make_async_copy(taby_hbm.at[0:2], tabyf, local_sem.at[4]),
        pltpu.make_async_copy(tabx_hbm, tabx, local_sem.at[5]),
        pltpu.make_async_copy(taby_hbm.at[2:4], tabyb, local_sem.at[6]),
    ]
    for load in loads:
        load.start()

    loads[1].wait()

    @pl.when(gy == 4)
    def _():
        for cc in range(6):
            for i in range(16):
                kn_out[cc, i : i + 1, 0:64] = kraw[cc, i, 0:1, :]

    kn = pltpu.make_async_remote_copy(
        src_ref=kn_out, dst_ref=kn_in, send_sem=kn_sems.at[0], recv_sem=kn_sems.at[1],
        device_id=by_y(0), device_id_type=MESH,
    )

    @pl.when(gy == 4)
    def _():
        kn.start()

    loads[0].wait()

    def z_forward(n):
        arrived(0, n, r1, 4)
        near = [r1[n, s].reshape(64, 128) for s in range(2)]
        far = [r1[n, s + 2].reshape(64, 128) for s in range(2)]
        out = [
            right_product(jnp.concatenate([a + b for a, b in zip(near, far)], axis=1), tabz, FORWARD),
            right_product(jnp.concatenate([a - b for a, b in zip(near, far)], axis=1), tabz, FORWARD + 1),
        ]
        for t in range(2):
            parts = swap_lanes(
                [out[i % 2][16 * (i // 2) : 16 * (i // 2) + 16, 128 * t : 128 * t + 128] for i in range(8)]
            )
            for q in range(8):
                s2[n, 4 * t + q // 2, 16 * (q % 2) : 16 * (q % 2) + 16, :] = parts[q]
        send_all(1, n, s2, r2, 8, gy, by_y)

    repeat(0, 3, z_forward)

    late = (gy >= 4).astype(jnp.int32)
    first = gy == 0

    @pl.when(first)
    def _():
        kn.wait_recv()

    for load in loads[2:4]:
        load.wait()
    far = first & (ac >= 8)
    middle = first & (lax.rem(ac, 8) == 0)

    def prepare(cc):
        for v in range(4):
            blocks = []
            for g in range(4):
                i = 4 * v + g
                even = kraw[cc, i, pl.ds(0, 16, stride=2), :]
                even = jnp.where(late == 1, kraw[cc, i, pl.ds(2, 16, stride=2), :], even)
                block = jnp.concatenate([even, kraw[cc, i, pl.ds(1, 16, stride=2), :]], axis=0)
                row = lax.broadcasted_iota(jnp.int32, block.shape, 0)
                nyquist = jnp.broadcast_to(kn_in[cc, i : i + 1, 0:64], block.shape)
                nyquist = jnp.where(first, nyquist, block)
                top = jnp.where(far, nyquist, block)
                if i == 0:
                    top = jnp.where(middle, 0.5 * (block + nyquist), top)
                    half = jnp.where(middle & (row == 0), 0.5 * (block - nyquist), 0.0)
                    half = jnp.concatenate([half, jnp.zeros((96, 64), F32)], axis=0)
                    k2[cc] = -INVERSE_COUNT * half.T
                blocks.append(jnp.where(row == 0, top, block))
            kp[cc, v] = -INVERSE_COUNT * jnp.concatenate(blocks, axis=0).T

    repeat(0, 6, prepare)
    lane = lax.broadcasted_iota(jnp.int32, (64, 128), 1)
    corner = jnp.where(middle & (lane == 0), 2.0 * EXCHANGE * INVERSE_COUNT, 0.0)
    for cc in range(3):
        k2[cc] += corner
        for v in range(4):
            kp[cc, v] += INVERSE_COUNT * (lamx[...] + lam[v : v + 1, :])

    repeat(3, 6, z_forward)

    for load in loads[4:]:
        load.wait()
    packed_lane = first & ((lax.broadcasted_iota(jnp.int32, (256, 128), 1) & 31) == 0)

    def y_forward(c):
        arrived(1, 2 * c, r2, 8)
        arrived(1, 2 * c + 1, r2, 8)
        both = [r2[pl.ds(2 * c, 2), 4 * h : 4 * h + 4].reshape(256, 128) for h in range(2)]
        out = []
        for parity, value in enumerate((both[0] + both[1], both[0] - both[1])):
            rows = left_product(tabyf, parity, value)
            out.append(jnp.where(packed_lane, rows[256:], rows[:256]))
        for part in range(2):
            at = [128 * part + 64 * (g // 2) for g in range(4)]
            parts = swap_lanes([out[g % 2][at[g] : at[g] + 64] for g in range(4)])
            for x in range(4):
                s3[c, pl.ds(4 * part + x, 64, stride=8), :] = parts[x]
        send_all(2, c, s3_blocks, r3, 16, ac, by_xz)

    s3_blocks = s3.reshape(3, 16, 32, 128)
    r4_blocks = r4.reshape(3, 16, 32, 128)
    repeat(0, 3, y_forward)

    def x_forward(c):
        arrived(2, c, r3, 16)
        tiles = [r3[c, :, 8 * v : 8 * v + 8, :].reshape(128, 128) for v in range(4)]
        for v in range(4):
            spec[c, v] = left_product(tabx, XF, tiles[v])
        spec[c, 4] = left_product(tabx, XM, tiles[0])

    repeat(0, 3, x_forward)

    for c in range(3):
        for v in range(4):
            terms = []
            for part in range(2):
                rows = slice(64 * part, 64 * part + 64)
                total = sum(kp[PAIR[c][d], v] * spec[d, v, rows, :] for d in range(3))
                if v == 0:
                    total = total + sum(k2[PAIR[c][d]] * spec[d, 4, rows, :] for d in range(3))
                terms.append(total)
            out = left_product(tabx, XB, jnp.concatenate(terms, axis=0))
            s4[c, :, 8 * v : 8 * v + 8, :] = out.reshape(16, 8, 128)
        send_all(3, c, s4, r4_blocks, 16, ac, by_xz)

    def y_backward(c):
        arrived(3, c, r4_blocks, 16)
        pieces = [
            swap_lanes([r4[c, pl.ds(4 * part + x, 64, stride=8), :] for x in range(4)]) for part in range(2)
        ]
        out = []
        for parity in range(2):
            value = [pieces[part][2 * g + parity] for part in range(2) for g in range(2)]
            rows = left_product(tabyb, parity, jnp.concatenate(value, axis=0))
            out.append(jnp.where(packed_lane, rows[256:], rows[:256]))
        for h, value in enumerate((out[0] + out[1], out[0] - out[1])):
            s5[pl.ds(2 * c, 2), 4 * h : 4 * h + 4] = value.reshape(2, 4, 32, 128)
        send_all(4, 2 * c, s5, r5, 8, gy, by_y)
        send_all(4, 2 * c + 1, s5, r5, 8, gy, by_y)

    repeat(0, 3, y_backward)

    def z_backward(n):
        arrived(4, n, r5, 8)
        tiles = [[], []]
        for t in range(2):
            parts = swap_lanes(
                [r5[n, 4 * t + q // 2, 16 * (q % 2) : 16 * (q % 2) + 16, :] for q in range(8)]
            )
            for parity in range(2):
                tiles[parity].append(jnp.concatenate(parts[parity::2], axis=0))
        out = [right_product(jnp.concatenate(tiles[p], axis=1), tabz, BACKWARD + p) for p in range(2)]
        for h, value in enumerate((out[0] + out[1], out[0] - out[1])):
            s6[n, 2 * h] = value[:, 0:128]
            s6[n, 2 * h + 1] = value[:, 128:256]
        send_all(5, n, s6, r6, 4, gz, by_z)

    repeat(0, 6, z_backward)
    repeat(0, 6, lambda n: arrived(5, n, r6, 4))

    def sent(e, src, chunks, count):
        def one(n):
            part = src.at[n, pl.ds(0, count - 1)]
            copy(e, n, part, part, by_y(lax.rem(gy + 1, 8))).wait_send()

        repeat(0, chunks, one)

    sent(0, r1, 6, 4)
    sent(1, s2, 6, 8)
    sent(2, s3_blocks, 3, 16)
    sent(3, s4, 3, 16)
    sent(4, s5, 6, 8)
    sent(5, s6, 6, 4)

    @pl.when(gy == 4)
    def _():
        kn.wait_send()


def advance(m, demag, applied, pred_hbm, torque_hbm, pout, tout, sems):
    cross = lambda a, b: [
        a[1] * b[2] - a[2] * b[1],
        a[2] * b[0] - a[0] * b[2],
        a[0] * b[1] - a[1] * b[0],
    ]
    stores = []
    for s in range(4):
        planes = slice(4 * s, 4 * s + 4)
        for half in range(2):
            rows = slice(16 * half, 16 * half + 16)
            mag = [m[c, planes, rows, :] for c in range(3)]
            field = [demag[2 * c + half, s].reshape(4, 16, 128) + applied[c] for c in range(3)]
            precess = cross(mag, field)
            twist = cross(mag, precess)
            torque = [-(precess[c] + DAMPING * twist[c]) / (1.0 + DAMPING * DAMPING) for c in range(3)]
            stepped = [mag[c] + STEP * torque[c] for c in range(3)]
            length = jnp.sqrt(stepped[0] * stepped[0] + stepped[1] * stepped[1] + stepped[2] * stepped[2])
            for c in range(3):
                tout[c, planes, rows, :] = torque[c]
                pout[c, planes, rows, :] = stepped[c] / length
        stores += [
            pltpu.make_async_copy(tout.at[:, planes], torque_hbm.at[:, planes], sems.at[s, 0]),
            pltpu.make_async_copy(pout.at[:, planes], pred_hbm.at[:, planes], sems.at[s, 1]),
        ]
        stores[-2].start()
        stores[-1].start()
    for store in stores:
        store.wait()


def shards(magnetization, kernel, applied):
    zf, zb = z_tables()
    yf, yb = y_tables()
    tabz = np.stack([halves(t) for t in zf + zb])
    taby = np.stack([halves(t) for t in yf + yb])
    tabx = np.stack([halves(t) for t in x_tables()])
    lam, lamx = eigen_tables()
    shape = magnetization.shape
    anywhere = pl.BlockSpec(memory_space=pltpu.HBM)
    in_vmem = pl.BlockSpec(memory_space=pltpu.VMEM)
    vmem = lambda *shape, dtype=F32: pltpu.VMEM(shape, dtype)
    m, demag = pl.pallas_call(
        transform,
        out_shape=[vmem(*shape), vmem(6, 4, 64, 128)],
        in_specs=[anywhere] * 7,
        out_specs=[in_vmem, in_vmem],
        scratch_shapes=[
            vmem(6, 16, 64, 64),
            vmem(4, 2, 256, 256, dtype=BF16),
            vmem(2, 2, 512, 256, dtype=BF16),
            vmem(2, 2, 512, 256, dtype=BF16),
            vmem(3, 2, 128, 128, dtype=BF16),
            vmem(4, 128),
            vmem(64, 128),
            vmem(6, 4, 64, 128),
            vmem(6, 64, 128),
            vmem(6, 16, 128),
            vmem(6, 16, 128),
            vmem(6, 4, 4, 16, 128),
            vmem(6, 8, 32, 128),
            vmem(6, 8, 32, 128),
            vmem(3, 512, 128),
            vmem(3, 16, 32, 128),
            vmem(3, 5, 128, 128),
            vmem(3, 16, 32, 128),
            vmem(3, 512, 128),
            vmem(6, 8, 32, 128),
            vmem(6, 8, 32, 128),
            vmem(6, 4, 64, 128),
            pltpu.SemaphoreType.DMA((7,)),
            pltpu.SemaphoreType.DMA((6, 6)),
            pltpu.SemaphoreType.DMA((6, 6)),
            pltpu.SemaphoreType.DMA((2,)),
        ],
        compiler_params=pltpu.CompilerParams(
            collective_id=0, has_side_effects=True, vmem_limit_bytes=40 * 1024 * 1024
        ),
    )(
        magnetization, kernel, jnp.asarray(tabz), jnp.asarray(taby), jnp.asarray(tabx),
        jnp.asarray(lam), jnp.asarray(lamx),
    )
    return pl.pallas_call(
        advance,
        out_shape=[jax.ShapeDtypeStruct(shape, F32)] * 2,
        in_specs=[in_vmem, in_vmem, pl.BlockSpec(memory_space=pltpu.SMEM)],
        out_specs=[anywhere] * 2,
        scratch_shapes=[vmem(*shape), vmem(*shape), pltpu.SemaphoreType.DMA((4, 2))],
        compiler_params=pltpu.CompilerParams(vmem_limit_bytes=16 * 1024 * 1024),
    )(m, demag, applied)


def solution(mesh):
    return jax.shard_map(
        shards,
        mesh=mesh,
        in_specs=(P(None, "gx", "gy", "gz"), P(None, ("gx", "gz"), "gy", None), P()),
        out_specs=(P(None, "gx", "gy", "gz"), P(None, "gx", "gy", "gz")),
        check_vma=False,
    )
```

```python
import math

import jax
import jax.numpy as jnp
import numpy as np
from jax import lax
from jax.experimental import pallas as pl
from jax.experimental.pallas import tpu as pltpu
from jax.sharding import PartitionSpec as P

MESH = pl.DeviceIdType.MESH
F32 = jnp.float32
BF16 = jnp.bfloat16
NX, NY, NZ = 64, 256, 512
EXCHANGE = 1.0
DAMPING = 0.3
STEP = 0.2
INVERSE_COUNT = 1.0 / (NX * NY * NZ)


def wave_z(block, slot):
    odd = slot >= 16
    return 64 * block + 2 * (slot % 16) + np.where(odd, 1, np.where(block >= 4, 2, 0))


def turn(rows, cols, length):
    angle = 2.0 * np.pi / length * ((rows[:, None] * cols[None, :]) % length)
    return np.cos(angle), np.sin(angle)


def grid(*counts):
    return [a.reshape(-1) for a in np.meshgrid(*(np.arange(n) for n in counts), indexing="ij")]


def z_tables():
    forward, backward = [], []
    for parity in range(2):
        block, part, slot = grid(8, 2, 16)
        cosine, sine = turn(np.arange(NZ // 2), wave_z(block, slot + 16 * parity), NZ)
        table = np.where(part == 0, cosine, -sine)
        weight = np.full(256, 2.0)
        if parity == 0:
            packed = (block == 0) & (slot == 0)
            alternate = 1.0 - 2.0 * (np.arange(NZ // 2) % 2)
            table[:, packed & (part == 1)] = alternate[:, None]
            weight[packed] = 1.0
        forward.append(table)
        backward.append(weight[:, None] * table.T)
    return forward, backward


def y_tables():
    forward, backward = [], []
    for parity in range(2):
        part, group, owner, tile = grid(2, 2, 16, 4)
        ky = 16 * owner + 4 * tile + 2 * group + parity
        half, block, yp, row = grid(2, 4, 2, 16)
        cosine, sine = turn(ky, 32 * block + 16 * half + row, NY)
        out_re, in_re = (part == 0)[:, None], (yp == 0)[None, :]
        plain = np.where(out_re == in_re, cosine, np.where(out_re, sine, -sine))
        low, high = ((ky > 0) & (ky < 128))[:, None], (ky > 128)[:, None]
        single = np.where(out_re, cosine, -sine)
        packed = np.where(low, np.where(in_re, single, 0.0), np.where(high, np.where(in_re, 0.0, single), plain))
        weight = np.where(low | high, 2.0, 1.0)
        forward.append(np.concatenate([plain, packed], axis=0))
        backward.append(np.concatenate([plain.T, (weight * packed).T], axis=0))
    return forward, backward


def x_tables():
    part, kx = grid(2, 64)
    owner, xp, xs = grid(16, 2, 4)
    cosine, sine = turn(kx, 4 * owner + xs, NX)
    out_re, in_re = (part == 0)[:, None], (xp == 0)[None, :]
    forward = np.where(out_re == in_re, cosine, np.where(out_re, sine, -sine))
    mirrored = np.where(in_re, forward, -forward)
    backward = np.where(out_re == in_re, cosine, np.where(in_re, -sine, sine)).T
    return forward, mirrored, backward


def eigen_tables():
    lam = lambda k, n: 2.0 * np.cos(2.0 * np.pi * k / n) - 2.0
    table = np.zeros((16, 8, 4, 128))
    for owner in range(16):
        for block in range(8):
            for tile in range(4):
                for group in range(4):
                    ky = 16 * owner + 4 * tile + group
                    kz = wave_z(block, np.arange(32))
                    row = lam(ky, NY) + lam(kz, NZ)
                    if block == 0:
                        row[0] = lam(ky, NY) + (-2.0 if ky % 128 == 0 else (-4.0 if ky > 128 else 0.0))
                    table[owner, block, tile, 32 * group : 32 * group + 32] = row
    return (
        (table * EXCHANGE).reshape(128, 4, 128).astype(np.float32),
        np.broadcast_to((lam(np.arange(64), NX) * EXCHANGE)[:, None], (64, 128)).astype(np.float32),
    )


def halves(table):
    table = np.asarray(table, np.float64)
    high = table.astype(np.float32).astype(jnp.bfloat16)
    low = (table - high.astype(np.float64)).astype(np.float32).astype(jnp.bfloat16)
    return np.stack([high, low])


def split(value):
    high = value.astype(BF16)
    return high, (value - high.astype(F32)).astype(BF16)


def dot(a, b):
    return jnp.dot(a, b, preferred_element_type=F32)


def right_product(value, table, index):
    high, low = split(value)
    rows = value.shape[0]
    both = dot(jnp.concatenate([high, low], axis=0), table[index, 0])
    return both[:rows] + both[rows:] + dot(high, table[index, 1])


def left_product(table, index, value):
    high, low = split(value)
    cols = value.shape[1]
    both = dot(table[index, 0], jnp.concatenate([high, low], axis=1))
    return both[:, :cols] + both[:, cols:] + dot(table[index, 1], high)


def swap_lanes(values):
    values = list(values)
    lane = lax.broadcasted_iota(jnp.int32, values[0].shape, 1)
    step = len(values) // 2
    width = 64
    while step:
        low = (lane & width) == 0
        for i in range(len(values)):
            if i & step == 0:
                a, b = values[i], values[i + step]
                values[i] = jnp.where(low, a, pltpu.roll(b, width, 1))
                values[i + step] = jnp.where(low, pltpu.roll(a, 128 - width, 1), b)
        step //= 2
        width //= 2
    return values


PAIR = ((0, 3, 4), (3, 1, 5), (4, 5, 2))
FORWARD, BACKWARD = 0, 2
XF, XM, XB = range(3)


def transform(
    m_hbm, k_hbm, tabz_hbm, taby_hbm, tabx_hbm, lam_hbm, lamx_hbm,
    m, r6,
    kraw, tabz, tabyf, tabyb, tabx, lam, lamx, kp, k2, kn_out, kn_in,
    r1, s2, r2, s3, r3, spec, s4, r4, s5, r5, s6,
    local_sem, send_sem, recv_sem, kn_sems,
):
    gx, gy, gz = lax.axis_index("gx"), lax.axis_index("gy"), lax.axis_index("gz")
    ac = gx * 4 + gz
    load_m = pltpu.make_async_copy(m_hbm, m, local_sem.at[0])
    load_m.start()

    by_z = lambda p: {"gz": p}
    by_y = lambda p: {"gy": p}
    by_xz = lambda p: {"gx": p // 4, "gz": lax.rem(p, 4)}

    barrier = pltpu.get_barrier_semaphore()

    def repeat(start, stop, step):
        def one(j, carry):
            step(j)
            return carry

        lax.fori_loop(start, stop, one, 0)

    def greet(count, me, place):
        repeat(
            1,
            count,
            lambda j: pl.semaphore_signal(
                barrier, inc=1, device_id=place(lax.rem(me + j, count)), device_id_type=MESH
            ),
        )

    greet(16, ac, by_xz)
    greet(8, gy, by_y)
    pl.semaphore_wait(barrier, 22)

    def copy(e, n, src, dst, device):
        return pltpu.make_async_remote_copy(
            src_ref=src, dst_ref=dst, send_sem=send_sem.at[e, n], recv_sem=recv_sem.at[e, n],
            device_id=device, device_id_type=MESH,
        )

    def send_all(e, n, src, dst, count, me, place):
        def one(j):
            p = lax.rem(me + j, count)
            copy(e, n, src.at[n, p], dst.at[n, me], place(p)).start()

        repeat(1, count, one)
        dst[n, me] = src[n, me]

    def arrived(e, n, dst, count):
        part = dst.at[n, pl.ds(0, count - 1)]
        copy(e, n, part, part, by_y(lax.rem(gy + 1, 8))).wait_recv()

    load_m.wait()
    m_blocks = m.reshape(3, 4, 4, 32, 128)

    def send_m(n):
        c, half = n // 2, lax.rem(n, 2)
        rows = pl.ds(pl.multiple_of(16 * half, 16), 16)

        def one(j):
            p = lax.rem(gz + j, 4)
            copy(0, n, m_blocks.at[c, p, :, rows, :], r1.at[n, gz], by_z(p)).start()

        repeat(1, 4, one)
        r1[n, gz] = m_blocks[c, gz, :, rows, :]

    repeat(0, 6, send_m)

    loads = [
        pltpu.make_async_copy(tabz_hbm, tabz, local_sem.at[0]),
        pltpu.make_async_copy(k_hbm, kraw, local_sem.at[1]),
        pltpu.make_async_copy(lam_hbm.at[ac * 8 + gy], lam, local_sem.at[2]),
        pltpu.make_async_copy(lamx_hbm, lamx, local_sem.at[3]),
        pltpu.make_async_copy(taby_hbm.at[0:2], tabyf, local_sem.at[4]),
        pltpu.make_async_copy(tabx_hbm, tabx, local_sem.at[5]),
        pltpu.make_async_copy(taby_hbm.at[2:4], tabyb, local_sem.at[6]),
    ]
    for load in loads:
        load.start()

    loads[1].wait()

    @pl.when(gy == 4)
    def _():
        for cc in range(6):
            for i in range(16):
                kn_out[cc, i : i + 1, 0:64] = kraw[cc, i, 0:1, :]

    kn = pltpu.make_async_remote_copy(
        src_ref=kn_out, dst_ref=kn_in, send_sem=kn_sems.at[0], recv_sem=kn_sems.at[1],
        device_id=by_y(0), device_id_type=MESH,
    )

    @pl.when(gy == 4)
    def _():
        kn.start()

    loads[0].wait()

    def z_forward(n):
        arrived(0, n, r1, 4)
        near = [r1[n, s].reshape(64, 128) for s in range(2)]
        far = [r1[n, s + 2].reshape(64, 128) for s in range(2)]
        out = [
            right_product(jnp.concatenate([a + b for a, b in zip(near, far)], axis=1), tabz, FORWARD),
            right_product(jnp.concatenate([a - b for a, b in zip(near, far)], axis=1), tabz, FORWARD + 1),
        ]
        for t in range(2):
            parts = swap_lanes(
                [out[i % 2][16 * (i // 2) : 16 * (i // 2) + 16, 128 * t : 128 * t + 128] for i in range(8)]
            )
            for q in range(8):
                s2[n, 4 * t + q // 2, 16 * (q % 2) : 16 * (q % 2) + 16, :] = parts[q]
        send_all(1, n, s2, r2, 8, gy, by_y)

    repeat(0, 3, z_forward)

    late = (gy >= 4).astype(jnp.int32)
    first = gy == 0

    @pl.when(first)
    def _():
        kn.wait_recv()

    for load in loads[2:4]:
        load.wait()
    far = first & (ac >= 8)
    middle = first & (lax.rem(ac, 8) == 0)

    def prepare(cc):
        for v in range(4):
            blocks = []
            for g in range(4):
                i = 4 * v + g
                even = kraw[cc, i, pl.ds(0, 16, stride=2), :]
                even = jnp.where(late == 1, kraw[cc, i, pl.ds(2, 16, stride=2), :], even)
                block = jnp.concatenate([even, kraw[cc, i, pl.ds(1, 16, stride=2), :]], axis=0)
                row = lax.broadcasted_iota(jnp.int32, block.shape, 0)
                nyquist = jnp.broadcast_to(kn_in[cc, i : i + 1, 0:64], block.shape)
                nyquist = jnp.where(first, nyquist, block)
                top = jnp.where(far, nyquist, block)
                if i == 0:
                    top = jnp.where(middle, 0.5 * (block + nyquist), top)
                    half = jnp.where(middle & (row == 0), 0.5 * (block - nyquist), 0.0)
                    half = jnp.concatenate([half, jnp.zeros((96, 64), F32)], axis=0)
                    k2[cc] = -INVERSE_COUNT * half.T
                blocks.append(jnp.where(row == 0, top, block))
            kp[cc, v] = -INVERSE_COUNT * jnp.concatenate(blocks, axis=0).T

    repeat(0, 6, prepare)
    lane = lax.broadcasted_iota(jnp.int32, (64, 128), 1)
    corner = jnp.where(middle & (lane == 0), 2.0 * EXCHANGE * INVERSE_COUNT, 0.0)
    for cc in range(3):
        k2[cc] += corner
        for v in range(4):
            kp[cc, v] += INVERSE_COUNT * (lamx[...] + lam[v : v + 1, :])

    repeat(3, 6, z_forward)

    for load in loads[4:]:
        load.wait()
    packed_lane = first & ((lax.broadcasted_iota(jnp.int32, (256, 128), 1) & 31) == 0)

    def y_forward(c):
        arrived(1, 2 * c, r2, 8)
        arrived(1, 2 * c + 1, r2, 8)
        both = [r2[pl.ds(2 * c, 2), 4 * h : 4 * h + 4].reshape(256, 128) for h in range(2)]
        out = []
        for parity, value in enumerate((both[0] + both[1], both[0] - both[1])):
            rows = left_product(tabyf, parity, value)
            out.append(jnp.where(packed_lane, rows[256:], rows[:256]))
        for part in range(2):
            at = [128 * part + 64 * (g // 2) for g in range(4)]
            parts = swap_lanes([out[g % 2][at[g] : at[g] + 64] for g in range(4)])
            for x in range(4):
                s3[c, pl.ds(4 * part + x, 64, stride=8), :] = parts[x]
        send_all(2, c, s3_blocks, r3, 16, ac, by_xz)

    s3_blocks = s3.reshape(3, 16, 32, 128)
    r4_blocks = r4.reshape(3, 16, 32, 128)
    repeat(0, 3, y_forward)

    def x_forward(c):
        arrived(2, c, r3, 16)
        tiles = [r3[c, :, 8 * v : 8 * v + 8, :].reshape(128, 128) for v in range(4)]
        for v in range(4):
            spec[c, v] = left_product(tabx, XF, tiles[v])
        spec[c, 4] = left_product(tabx, XM, tiles[0])

    repeat(0, 3, x_forward)

    for c in range(3):
        for v in range(4):
            terms = []
            for part in range(2):
                rows = slice(64 * part, 64 * part + 64)
                total = sum(kp[PAIR[c][d], v] * spec[d, v, rows, :] for d in range(3))
                if v == 0:
                    total = total + sum(k2[PAIR[c][d]] * spec[d, 4, rows, :] for d in range(3))
                terms.append(total)
            out = left_product(tabx, XB, jnp.concatenate(terms, axis=0))
            s4[c, :, 8 * v : 8 * v + 8, :] = out.reshape(16, 8, 128)
        send_all(3, c, s4, r4_blocks, 16, ac, by_xz)

    def y_backward(c):
        arrived(3, c, r4_blocks, 16)
        pieces = [
            swap_lanes([r4[c, pl.ds(4 * part + x, 64, stride=8), :] for x in range(4)]) for part in range(2)
        ]
        out = []
        for parity in range(2):
            value = [pieces[part][2 * g + parity] for part in range(2) for g in range(2)]
            rows = left_product(tabyb, parity, jnp.concatenate(value, axis=0))
            out.append(jnp.where(packed_lane, rows[256:], rows[:256]))
        for h, value in enumerate((out[0] + out[1], out[0] - out[1])):
            s5[pl.ds(2 * c, 2), 4 * h : 4 * h + 4] = value.reshape(2, 4, 32, 128)
        send_all(4, 2 * c, s5, r5, 8, gy, by_y)
        send_all(4, 2 * c + 1, s5, r5, 8, gy, by_y)

    repeat(0, 3, y_backward)

    def z_backward(n):
        arrived(4, n, r5, 8)
        tiles = [[], []]
        for t in range(2):
            parts = swap_lanes(
                [r5[n, 4 * t + q // 2, 16 * (q % 2) : 16 * (q % 2) + 16, :] for q in range(8)]
            )
            for parity in range(2):
                tiles[parity].append(jnp.concatenate(parts[parity::2], axis=0))
        out = [right_product(jnp.concatenate(tiles[p], axis=1), tabz, BACKWARD + p) for p in range(2)]
        for h, value in enumerate((out[0] + out[1], out[0] - out[1])):
            s6[n, 2 * h] = value[:, 0:128]
            s6[n, 2 * h + 1] = value[:, 128:256]
        send_all(5, n, s6, r6, 4, gz, by_z)

    repeat(0, 6, z_backward)
    repeat(0, 6, lambda n: arrived(5, n, r6, 4))

    def sent(e, src, chunks, count):
        def one(n):
            part = src.at[n, pl.ds(0, count - 1)]
            copy(e, n, part, part, by_y(lax.rem(gy + 1, 8))).wait_send()

        repeat(0, chunks, one)

    sent(0, r1, 6, 4)
    sent(1, s2, 6, 8)
    sent(2, s3_blocks, 3, 16)
    sent(3, s4, 3, 16)
    sent(4, s5, 6, 8)
    sent(5, s6, 6, 4)

    @pl.when(gy == 4)
    def _():
        kn.wait_send()


def advance(m, demag, applied, pred_hbm, torque_hbm, pout, tout, sems):
    cross = lambda a, b: [
        a[1] * b[2] - a[2] * b[1],
        a[2] * b[0] - a[0] * b[2],
        a[0] * b[1] - a[1] * b[0],
    ]
    stores = []
    for s in range(4):
        planes = slice(4 * s, 4 * s + 4)
        for half in range(2):
            rows = slice(16 * half, 16 * half + 16)
            mag = [m[c, planes, rows, :] for c in range(3)]
            field = [demag[2 * c + half, s].reshape(4, 16, 128) + applied[c] for c in range(3)]
            precess = cross(mag, field)
            twist = cross(mag, precess)
            torque = [-(precess[c] + DAMPING * twist[c]) / (1.0 + DAMPING * DAMPING) for c in range(3)]
            stepped = [mag[c] + STEP * torque[c] for c in range(3)]
            length = jnp.sqrt(stepped[0] * stepped[0] + stepped[1] * stepped[1] + stepped[2] * stepped[2])
            for c in range(3):
                tout[c, planes, rows, :] = torque[c]
                pout[c, planes, rows, :] = stepped[c] / length
        stores += [
            pltpu.make_async_copy(tout.at[:, planes], torque_hbm.at[:, planes], sems.at[s, 0]),
            pltpu.make_async_copy(pout.at[:, planes], pred_hbm.at[:, planes], sems.at[s, 1]),
        ]
        stores[-2].start()
        stores[-1].start()
    for store in stores:
        store.wait()


def shards(magnetization, kernel, applied):
    zf, zb = z_tables()
    yf, yb = y_tables()
    tabz = np.stack([halves(t) for t in zf + zb])
    taby = np.stack([halves(t) for t in yf + yb])
    tabx = np.stack([halves(t) for t in x_tables()])
    lam, lamx = eigen_tables()
    shape = magnetization.shape
    anywhere = pl.BlockSpec(memory_space=pltpu.HBM)
    in_vmem = pl.BlockSpec(memory_space=pltpu.VMEM)
    vmem = lambda *shape, dtype=F32: pltpu.VMEM(shape, dtype)
    m, demag = pl.pallas_call(
        transform,
        out_shape=[vmem(*shape), vmem(6, 4, 64, 128)],
        in_specs=[anywhere] * 7,
        out_specs=[in_vmem, in_vmem],
        scratch_shapes=[
            vmem(6, 16, 64, 64),
            vmem(4, 2, 256, 256, dtype=BF16),
            vmem(2, 2, 512, 256, dtype=BF16),
            vmem(2, 2, 512, 256, dtype=BF16),
            vmem(3, 2, 128, 128, dtype=BF16),
            vmem(4, 128),
            vmem(64, 128),
            vmem(6, 4, 64, 128),
            vmem(6, 64, 128),
            vmem(6, 16, 128),
            vmem(6, 16, 128),
            vmem(6, 4, 4, 16, 128),
            vmem(6, 8, 32, 128),
            vmem(6, 8, 32, 128),
            vmem(3, 512, 128),
            vmem(3, 16, 32, 128),
            vmem(3, 5, 128, 128),
            vmem(3, 16, 32, 128),
            vmem(3, 512, 128),
            vmem(6, 8, 32, 128),
            vmem(6, 8, 32, 128),
            vmem(6, 4, 64, 128),
            pltpu.SemaphoreType.DMA((7,)),
            pltpu.SemaphoreType.DMA((6, 6)),
            pltpu.SemaphoreType.DMA((6, 6)),
            pltpu.SemaphoreType.DMA((2,)),
        ],
        compiler_params=pltpu.CompilerParams(
            collective_id=0, has_side_effects=True, vmem_limit_bytes=62 * 1024 * 1024
        ),
    )(
        magnetization, kernel, jnp.asarray(tabz), jnp.asarray(taby), jnp.asarray(tabx),
        jnp.asarray(lam), jnp.asarray(lamx),
    )
    return pl.pallas_call(
        advance,
        out_shape=[jax.ShapeDtypeStruct(shape, F32)] * 2,
        in_specs=[in_vmem, in_vmem, pl.BlockSpec(memory_space=pltpu.SMEM)],
        out_specs=[anywhere] * 2,
        scratch_shapes=[vmem(*shape), vmem(*shape), pltpu.SemaphoreType.DMA((4, 2))],
        compiler_params=pltpu.CompilerParams(vmem_limit_bytes=16 * 1024 * 1024),
    )(m, demag, applied)


def solution(mesh):
    return jax.shard_map(
        shards,
        mesh=mesh,
        in_specs=(P(None, "gx", "gy", "gz"), P(None, ("gx", "gz"), "gy", None), P()),
        out_specs=(P(None, "gx", "gy", "gz"), P(None, "gx", "gy", "gz")),
        check_vma=False,
    )
```

```python
import math

import jax
import jax.numpy as jnp
import numpy as np
from jax import lax
from jax.experimental import pallas as pl
from jax.experimental.pallas import tpu as pltpu
from jax.sharding import PartitionSpec as P

MESH = pl.DeviceIdType.MESH
F32 = jnp.float32
BF16 = jnp.bfloat16
NX, NY, NZ = 64, 256, 512
EXCHANGE = 1.0
DAMPING = 0.3
STEP = 0.2
INVERSE_COUNT = 1.0 / (NX * NY * NZ)


def wave_z(block, slot):
    odd = slot >= 16
    return 64 * block + 2 * (slot % 16) + np.where(odd, 1, np.where(block >= 4, 2, 0))


def turn(rows, cols, length):
    angle = 2.0 * np.pi / length * ((rows[:, None] * cols[None, :]) % length)
    return np.cos(angle), np.sin(angle)


def grid(*counts):
    return [a.reshape(-1) for a in np.meshgrid(*(np.arange(n) for n in counts), indexing="ij")]


def z_tables():
    forward, backward = [], []
    for parity in range(2):
        block, part, slot = grid(8, 2, 16)
        cosine, sine = turn(np.arange(NZ // 2), wave_z(block, slot + 16 * parity), NZ)
        table = np.where(part == 0, cosine, -sine)
        weight = np.full(256, 2.0)
        if parity == 0:
            packed = (block == 0) & (slot == 0)
            alternate = 1.0 - 2.0 * (np.arange(NZ // 2) % 2)
            table[:, packed & (part == 1)] = alternate[:, None]
            weight[packed] = 1.0
        forward.append(table)
        backward.append(weight[:, None] * table.T)
    return forward, backward


def y_tables():
    forward, backward = [], []
    for parity in range(2):
        part, group, owner, tile = grid(2, 2, 16, 4)
        ky = 16 * owner + 4 * tile + 2 * group + parity
        half, block, yp, row = grid(2, 4, 2, 16)
        cosine, sine = turn(ky, 32 * block + 16 * half + row, NY)
        out_re, in_re = (part == 0)[:, None], (yp == 0)[None, :]
        plain = np.where(out_re == in_re, cosine, np.where(out_re, sine, -sine))
        low, high = ((ky > 0) & (ky < 128))[:, None], (ky > 128)[:, None]
        single = np.where(out_re, cosine, -sine)
        packed = np.where(low, np.where(in_re, single, 0.0), np.where(high, np.where(in_re, 0.0, single), plain))
        weight = np.where(low | high, 2.0, 1.0)
        forward.append(np.concatenate([plain, packed], axis=0))
        backward.append(np.concatenate([plain.T, (weight * packed).T], axis=0))
    return forward, backward


def x_tables():
    part, kx = grid(2, 64)
    owner, xp, xs = grid(16, 2, 4)
    cosine, sine = turn(kx, 4 * owner + xs, NX)
    out_re, in_re = (part == 0)[:, None], (xp == 0)[None, :]
    forward = np.where(out_re == in_re, cosine, np.where(out_re, sine, -sine))
    mirrored = np.where(in_re, forward, -forward)
    backward = np.where(out_re == in_re, cosine, np.where(in_re, -sine, sine)).T
    return forward, mirrored, backward


def eigen_tables():
    lam = lambda k, n: 2.0 * np.cos(2.0 * np.pi * k / n) - 2.0
    table = np.zeros((16, 8, 4, 128))
    for owner in range(16):
        for block in range(8):
            for tile in range(4):
                for group in range(4):
                    ky = 16 * owner + 4 * tile + group
                    kz = wave_z(block, np.arange(32))
                    row = lam(ky, NY) + lam(kz, NZ)
                    if block == 0:
                        row[0] = lam(ky, NY) + (-2.0 if ky % 128 == 0 else (-4.0 if ky > 128 else 0.0))
                    table[owner, block, tile, 32 * group : 32 * group + 32] = row
    return (
        (table * EXCHANGE).reshape(128, 4, 128).astype(np.float32),
        np.broadcast_to((lam(np.arange(64), NX) * EXCHANGE)[:, None], (64, 128)).astype(np.float32),
    )


def halves(table):
    table = np.asarray(table, np.float64)
    high = table.astype(np.float32).astype(jnp.bfloat16)
    low = (table - high.astype(np.float64)).astype(np.float32).astype(jnp.bfloat16)
    return np.stack([high, low])


def split(value):
    high = value.astype(BF16)
    return high, (value - high.astype(F32)).astype(BF16)


def dot(a, b):
    return jnp.dot(a, b, preferred_element_type=F32)


def right_product(value, table, index):
    high, low = split(value)
    rows = value.shape[0]
    both = dot(jnp.concatenate([high, low], axis=0), table[index, 0])
    return both[:rows] + both[rows:] + dot(high, table[index, 1])


def left_product(table, index, value):
    high, low = split(value)
    cols = value.shape[1]
    both = dot(table[index, 0], jnp.concatenate([high, low], axis=1))
    return both[:, :cols] + both[:, cols:] + dot(table[index, 1], high)


def swap_lanes(values):
    values = list(values)
    lane = lax.broadcasted_iota(jnp.int32, values[0].shape, 1)
    step = len(values) // 2
    width = 64
    while step:
        low = (lane & width) == 0
        for i in range(len(values)):
            if i & step == 0:
                a, b = values[i], values[i + step]
                values[i] = jnp.where(low, a, pltpu.roll(b, width, 1))
                values[i + step] = jnp.where(low, pltpu.roll(a, 128 - width, 1), b)
        step //= 2
        width //= 2
    return values


PAIR = ((0, 3, 4), (3, 1, 5), (4, 5, 2))
FORWARD, BACKWARD = 0, 2
XF, XM, XB = range(3)


def transform(
    m_hbm, k_hbm, tabz_hbm, taby_hbm, tabx_hbm, lam_hbm, lamx_hbm,
    m, r6,
    kraw, tabz, tabyf, tabyb, tabx, lam, lamx, kp, k2, kn_out, kn_in,
    r1, s2, r2, s3, r3, spec, s4, r4, s5, r5, s6,
    local_sem, send_sem, recv_sem, kn_sems,
):
    gx, gy, gz = lax.axis_index("gx"), lax.axis_index("gy"), lax.axis_index("gz")
    ac = gx * 4 + gz
    load_m = pltpu.make_async_copy(m_hbm, m, local_sem.at[0])
    load_m.start()

    by_y = lambda p: {"gy": p}
    on_z = [(z, {"gz": z}) for z in (lax.rem(gz + d, 4) for d in (2, 1, 3))]
    on_y = [
        (y, {"gy": y})
        for y in (
            4 * lax.rem(gy // 4 + p, 2) + lax.rem(gy + d, 4)
            for p, d in ((1, 2), (1, 1), (1, 3), (1, 0), (0, 2), (0, 1), (0, 3))
        )
    ]
    on_xz = [
        (4 * x + z, {"gx": x, "gz": z})
        for x, z in (
            (2 * lax.rem(gx // 2 + p, 2) + lax.rem(gx + k, 2), lax.rem(gz + d, 4))
            for p in (1, 0)
            for d in (2, 1, 3, 0)
            for k in (0, 1)
            if (p, d, k) != (0, 0, 0)
        )
    ]

    barrier = pltpu.get_barrier_semaphore()

    def repeat(start, stop, step):
        def one(j, carry):
            step(j)
            return carry

        lax.fori_loop(start, stop, one, 0)

    for _, device in on_y + on_xz:
        pl.semaphore_signal(barrier, inc=1, device_id=device, device_id_type=MESH)
    pl.semaphore_wait(barrier, 22)

    def copy(e, n, src, dst, device):
        return pltpu.make_async_remote_copy(
            src_ref=src, dst_ref=dst, send_sem=send_sem.at[e, n], recv_sem=recv_sem.at[e, n],
            device_id=device, device_id_type=MESH,
        )

    def send_all(e, n, src, dst, me, others):
        for p, device in others:
            copy(e, n, src.at[n, p], dst.at[n, me], device).start()
        dst[n, me] = src[n, me]

    def arrived(e, n, dst, count):
        part = dst.at[n, pl.ds(0, count - 1)]
        copy(e, n, part, part, by_y(lax.rem(gy + 1, 8))).wait_recv()

    load_m.wait()
    m_blocks = m.reshape(3, 4, 4, 32, 128)

    def send_m(n):
        c, half = n // 2, lax.rem(n, 2)
        rows = pl.ds(pl.multiple_of(16 * half, 16), 16)

        for p, device in on_z:
            copy(0, n, m_blocks.at[c, p, :, rows, :], r1.at[n, gz], device).start()
        r1[n, gz] = m_blocks[c, gz, :, rows, :]

    repeat(0, 6, send_m)

    loads = [
        pltpu.make_async_copy(tabz_hbm, tabz, local_sem.at[0]),
        pltpu.make_async_copy(k_hbm, kraw, local_sem.at[1]),
        pltpu.make_async_copy(lam_hbm.at[ac * 8 + gy], lam, local_sem.at[2]),
        pltpu.make_async_copy(lamx_hbm, lamx, local_sem.at[3]),
        pltpu.make_async_copy(taby_hbm.at[0:2], tabyf, local_sem.at[4]),
        pltpu.make_async_copy(tabx_hbm, tabx, local_sem.at[5]),
        pltpu.make_async_copy(taby_hbm.at[2:4], tabyb, local_sem.at[6]),
    ]
    for load in loads:
        load.start()

    loads[1].wait()

    @pl.when(gy == 4)
    def _():
        for cc in range(6):
            for i in range(16):
                kn_out[cc, i : i + 1, 0:64] = kraw[cc, i, 0:1, :]

    kn = pltpu.make_async_remote_copy(
        src_ref=kn_out, dst_ref=kn_in, send_sem=kn_sems.at[0], recv_sem=kn_sems.at[1],
        device_id=by_y(0), device_id_type=MESH,
    )

    @pl.when(gy == 4)
    def _():
        kn.start()

    loads[0].wait()

    def z_forward(n):
        arrived(0, n, r1, 4)
        near = [r1[n, s].reshape(64, 128) for s in range(2)]
        far = [r1[n, s + 2].reshape(64, 128) for s in range(2)]
        out = [
            right_product(jnp.concatenate([a + b for a, b in zip(near, far)], axis=1), tabz, FORWARD),
            right_product(jnp.concatenate([a - b for a, b in zip(near, far)], axis=1), tabz, FORWARD + 1),
        ]
        for t in range(2):
            parts = swap_lanes(
                [out[i % 2][16 * (i // 2) : 16 * (i // 2) + 16, 128 * t : 128 * t + 128] for i in range(8)]
            )
            for q in range(8):
                s2[n, 4 * t + q // 2, 16 * (q % 2) : 16 * (q % 2) + 16, :] = parts[q]
        send_all(1, n, s2, r2, gy, on_y)

    repeat(0, 3, z_forward)

    late = (gy >= 4).astype(jnp.int32)
    first = gy == 0

    @pl.when(first)
    def _():
        kn.wait_recv()

    for load in loads[2:4]:
        load.wait()
    far = first & (ac >= 8)
    middle = first & (lax.rem(ac, 8) == 0)

    def prepare(cc):
        for v in range(4):
            blocks = []
            for g in range(4):
                i = 4 * v + g
                even = kraw[cc, i, pl.ds(0, 16, stride=2), :]
                even = jnp.where(late == 1, kraw[cc, i, pl.ds(2, 16, stride=2), :], even)
                block = jnp.concatenate([even, kraw[cc, i, pl.ds(1, 16, stride=2), :]], axis=0)
                row = lax.broadcasted_iota(jnp.int32, block.shape, 0)
                nyquist = jnp.broadcast_to(kn_in[cc, i : i + 1, 0:64], block.shape)
                nyquist = jnp.where(first, nyquist, block)
                top = jnp.where(far, nyquist, block)
                if i == 0:
                    top = jnp.where(middle, 0.5 * (block + nyquist), top)
                    half = jnp.where(middle & (row == 0), 0.5 * (block - nyquist), 0.0)
                    half = jnp.concatenate([half, jnp.zeros((96, 64), F32)], axis=0)
                    k2[cc] = -INVERSE_COUNT * half.T
                blocks.append(jnp.where(row == 0, top, block))
            kp[cc, v] = -INVERSE_COUNT * jnp.concatenate(blocks, axis=0).T

    repeat(0, 6, prepare)
    lane = lax.broadcasted_iota(jnp.int32, (64, 128), 1)
    corner = jnp.where(middle & (lane == 0), 2.0 * EXCHANGE * INVERSE_COUNT, 0.0)
    for cc in range(3):
        k2[cc] += corner
        for v in range(4):
            kp[cc, v] += INVERSE_COUNT * (lamx[...] + lam[v : v + 1, :])

    repeat(3, 6, z_forward)

    for load in loads[4:]:
        load.wait()
    packed_lane = first & ((lax.broadcasted_iota(jnp.int32, (256, 128), 1) & 31) == 0)

    def y_forward(c):
        arrived(1, 2 * c, r2, 8)
        arrived(1, 2 * c + 1, r2, 8)
        both = [r2[pl.ds(2 * c, 2), 4 * h : 4 * h + 4].reshape(256, 128) for h in range(2)]
        out = []
        for parity, value in enumerate((both[0] + both[1], both[0] - both[1])):
            rows = left_product(tabyf, parity, value)
            out.append(jnp.where(packed_lane, rows[256:], rows[:256]))
        for part in range(2):
            at = [128 * part + 64 * (g // 2) for g in range(4)]
            parts = swap_lanes([out[g % 2][at[g] : at[g] + 64] for g in range(4)])
            for x in range(4):
                s3[c, pl.ds(4 * part + x, 64, stride=8), :] = parts[x]
        send_all(2, c, s3_blocks, r3, ac, on_xz)

    s3_blocks = s3.reshape(3, 16, 32, 128)
    r4_blocks = r4.reshape(3, 16, 32, 128)
    repeat(0, 3, y_forward)

    def x_forward(c):
        arrived(2, c, r3, 16)
        tiles = [r3[c, :, 8 * v : 8 * v + 8, :].reshape(128, 128) for v in range(4)]
        for v in range(4):
            spec[c, v] = left_product(tabx, XF, tiles[v])
        spec[c, 4] = left_product(tabx, XM, tiles[0])

    repeat(0, 3, x_forward)

    for c in range(3):
        for v in range(4):
            terms = []
            for part in range(2):
                rows = slice(64 * part, 64 * part + 64)
                total = sum(kp[PAIR[c][d], v] * spec[d, v, rows, :] for d in range(3))
                if v == 0:
                    total = total + sum(k2[PAIR[c][d]] * spec[d, 4, rows, :] for d in range(3))
                terms.append(total)
            out = left_product(tabx, XB, jnp.concatenate(terms, axis=0))
            s4[c, :, 8 * v : 8 * v + 8, :] = out.reshape(16, 8, 128)
        send_all(3, c, s4, r4_blocks, ac, on_xz)

    def y_backward(c):
        arrived(3, c, r4_blocks, 16)
        pieces = [
            swap_lanes([r4[c, pl.ds(4 * part + x, 64, stride=8), :] for x in range(4)]) for part in range(2)
        ]
        out = []
        for parity in range(2):
            value = [pieces[part][2 * g + parity] for part in range(2) for g in range(2)]
            rows = left_product(tabyb, parity, jnp.concatenate(value, axis=0))
            out.append(jnp.where(packed_lane, rows[256:], rows[:256]))
        for h, value in enumerate((out[0] + out[1], out[0] - out[1])):
            s5[pl.ds(2 * c, 2), 4 * h : 4 * h + 4] = value.reshape(2, 4, 32, 128)
        send_all(4, 2 * c, s5, r5, gy, on_y)
        send_all(4, 2 * c + 1, s5, r5, gy, on_y)

    repeat(0, 3, y_backward)

    def z_backward(n):
        arrived(4, n, r5, 8)
        tiles = [[], []]
        for t in range(2):
            parts = swap_lanes(
                [r5[n, 4 * t + q // 2, 16 * (q % 2) : 16 * (q % 2) + 16, :] for q in range(8)]
            )
            for parity in range(2):
                tiles[parity].append(jnp.concatenate(parts[parity::2], axis=0))
        out = [right_product(jnp.concatenate(tiles[p], axis=1), tabz, BACKWARD + p) for p in range(2)]
        for h, value in enumerate((out[0] + out[1], out[0] - out[1])):
            s6[n, 2 * h] = value[:, 0:128]
            s6[n, 2 * h + 1] = value[:, 128:256]
        send_all(5, n, s6, r6, gz, on_z)

    repeat(0, 6, z_backward)

    def sent(e, src, chunks, count):
        def one(n):
            part = src.at[n, pl.ds(0, count - 1)]
            copy(e, n, part, part, by_y(lax.rem(gy + 1, 8))).wait_send()

        repeat(0, chunks, one)

    sent(0, r1, 6, 4)
    sent(1, s2, 6, 8)
    sent(2, s3_blocks, 3, 16)
    sent(3, s4, 3, 16)
    sent(4, s5, 6, 8)

    @pl.when(gy == 4)
    def _():
        kn.wait_send()

    repeat(0, 6, lambda n: arrived(5, n, r6, 4))
    sent(5, s6, 6, 4)


def advance(m, demag, applied, pred_hbm, torque_hbm, pout, tout, sems):
    cross = lambda a, b: [
        a[1] * b[2] - a[2] * b[1],
        a[2] * b[0] - a[0] * b[2],
        a[0] * b[1] - a[1] * b[0],
    ]
    stores = []
    for s in range(4):
        planes = slice(4 * s, 4 * s + 4)
        for half in range(2):
            rows = slice(16 * half, 16 * half + 16)
            mag = [m[c, planes, rows, :] for c in range(3)]
            field = [demag[2 * c + half, s].reshape(4, 16, 128) + applied[c] for c in range(3)]
            precess = cross(mag, field)
            twist = cross(mag, precess)
            torque = [-(precess[c] + DAMPING * twist[c]) / (1.0 + DAMPING * DAMPING) for c in range(3)]
            stepped = [mag[c] + STEP * torque[c] for c in range(3)]
            length = jnp.sqrt(stepped[0] * stepped[0] + stepped[1] * stepped[1] + stepped[2] * stepped[2])
            for c in range(3):
                tout[c, planes, rows, :] = torque[c]
                pout[c, planes, rows, :] = stepped[c] / length
        stores += [
            pltpu.make_async_copy(tout.at[:, planes], torque_hbm.at[:, planes], sems.at[s, 0]),
            pltpu.make_async_copy(pout.at[:, planes], pred_hbm.at[:, planes], sems.at[s, 1]),
        ]
        stores[-2].start()
        stores[-1].start()
    for store in stores:
        store.wait()


def shards(magnetization, kernel, applied):
    zf, zb = z_tables()
    yf, yb = y_tables()
    tabz = np.stack([halves(t) for t in zf + zb])
    taby = np.stack([halves(t) for t in yf + yb])
    tabx = np.stack([halves(t) for t in x_tables()])
    lam, lamx = eigen_tables()
    shape = magnetization.shape
    anywhere = pl.BlockSpec(memory_space=pltpu.HBM)
    in_vmem = pl.BlockSpec(memory_space=pltpu.VMEM)
    vmem = lambda *shape, dtype=F32: pltpu.VMEM(shape, dtype)
    m, demag = pl.pallas_call(
        transform,
        out_shape=[vmem(*shape), vmem(6, 4, 64, 128)],
        in_specs=[anywhere] * 7,
        out_specs=[in_vmem, in_vmem],
        scratch_shapes=[
            vmem(6, 16, 64, 64),
            vmem(4, 2, 256, 256, dtype=BF16),
            vmem(2, 2, 512, 256, dtype=BF16),
            vmem(2, 2, 512, 256, dtype=BF16),
            vmem(3, 2, 128, 128, dtype=BF16),
            vmem(4, 128),
            vmem(64, 128),
            vmem(6, 4, 64, 128),
            vmem(6, 64, 128),
            vmem(6, 16, 128),
            vmem(6, 16, 128),
            vmem(6, 4, 4, 16, 128),
            vmem(6, 8, 32, 128),
            vmem(6, 8, 32, 128),
            vmem(3, 512, 128),
            vmem(3, 16, 32, 128),
            vmem(3, 5, 128, 128),
            vmem(3, 16, 32, 128),
            vmem(3, 512, 128),
            vmem(6, 8, 32, 128),
            vmem(6, 8, 32, 128),
            vmem(6, 4, 64, 128),
            pltpu.SemaphoreType.DMA((7,)),
            pltpu.SemaphoreType.DMA((6, 6)),
            pltpu.SemaphoreType.DMA((6, 6)),
            pltpu.SemaphoreType.DMA((2,)),
        ],
        compiler_params=pltpu.CompilerParams(
            collective_id=0, has_side_effects=True, vmem_limit_bytes=62 * 1024 * 1024
        ),
    )(
        magnetization, kernel, jnp.asarray(tabz), jnp.asarray(taby), jnp.asarray(tabx),
        jnp.asarray(lam), jnp.asarray(lamx),
    )
    return pl.pallas_call(
        advance,
        out_shape=[jax.ShapeDtypeStruct(shape, F32)] * 2,
        in_specs=[in_vmem, in_vmem, pl.BlockSpec(memory_space=pltpu.SMEM)],
        out_specs=[anywhere] * 2,
        scratch_shapes=[vmem(*shape), vmem(*shape), pltpu.SemaphoreType.DMA((4, 2))],
        compiler_params=pltpu.CompilerParams(vmem_limit_bytes=16 * 1024 * 1024),
    )(m, demag, applied)


def solution(mesh):
    return jax.shard_map(
        shards,
        mesh=mesh,
        in_specs=(P(None, "gx", "gy", "gz"), P(None, ("gx", "gz"), "gy", None), P()),
        out_specs=(P(None, "gx", "gy", "gz"), P(None, "gx", "gy", "gz")),
        check_vma=False,
    )
```

```python
import math

import jax
import jax.numpy as jnp
import numpy as np
from jax import lax
from jax.experimental import pallas as pl
from jax.experimental.pallas import tpu as pltpu
from jax.sharding import PartitionSpec as P

MESH = pl.DeviceIdType.MESH
F32 = jnp.float32
BF16 = jnp.bfloat16
NX, NY, NZ = 64, 256, 512
EXCHANGE = 1.0
DAMPING = 0.3
STEP = 0.2
INVERSE_COUNT = 1.0 / (NX * NY * NZ)


def wave_z(block, slot):
    odd = slot >= 16
    return 64 * block + 2 * (slot % 16) + np.where(odd, 1, np.where(block >= 4, 2, 0))


def turn(rows, cols, length):
    angle = 2.0 * np.pi / length * ((rows[:, None] * cols[None, :]) % length)
    return np.cos(angle), np.sin(angle)


def grid(*counts):
    return [a.reshape(-1) for a in np.meshgrid(*(np.arange(n) for n in counts), indexing="ij")]


def z_tables():
    forward, backward = [], []
    for parity in range(2):
        block, part, slot = grid(8, 2, 16)
        cosine, sine = turn(np.arange(NZ // 2), wave_z(block, slot + 16 * parity), NZ)
        table = np.where(part == 0, cosine, -sine)
        weight = np.full(256, 2.0)
        if parity == 0:
            packed = (block == 0) & (slot == 0)
            alternate = 1.0 - 2.0 * (np.arange(NZ // 2) % 2)
            table[:, packed & (part == 1)] = alternate[:, None]
            weight[packed] = 1.0
        forward.append(table)
        backward.append(weight[:, None] * table.T)
    return forward, backward


def wave_y(owner, tile, group):
    return 128 * (tile // 2) + 16 * owner + 8 * (tile % 2) + group


def y_tables():
    forward, backward = [], []
    for parity in range(2):
        group, owner, tile = grid(4, 8, 4)
        half, block, row = grid(2, 4, 16)
        tables = turn(wave_y(owner, tile, 2 * group + parity), 32 * block + 16 * half + row, NY)
        forward.append(np.concatenate(tables, axis=0))
        backward.append(np.concatenate([t.T for t in tables], axis=0))
    return forward, backward


def x_tables():
    part, kx = grid(2, 64)
    parity, owner, xs, xp = grid(2, 8, 4, 2)
    cosine, sine = turn(kx, 4 * owner + xs, NX)
    out_re, in_re = (part == 0)[:, None], (xp == 0)[None, :]
    mine = kx[:, None] % 2 == parity[None, :]
    forward = np.where(mine, np.where(out_re == in_re, cosine, np.where(out_re, sine, -sine)), 0.0)
    mirrored = np.where(in_re, forward, -forward)
    backward = np.where(mine, np.where(out_re == in_re, cosine, np.where(in_re, -sine, sine)), 0.0).T
    return forward, mirrored, backward


def eigen_tables():
    lam = lambda k, n: 2.0 * np.cos(2.0 * np.pi * k / n) - 2.0
    owner, parity, block, tile, group, slot = grid(8, 2, 8, 4, 8, 16)
    ky, kz = wave_y(owner, tile, group), wave_z(block, slot + 16 * parity)
    z_part = lam(kz, NZ)
    packed = (block == 0) & (parity == 0) & (slot == 0)
    z_part = np.where(packed, np.where(ky % 128 == 0, -2.0, np.where(ky > 128, -4.0, 0.0)), z_part)
    table = (lam(ky, NY) + z_part) * EXCHANGE
    return (
        table.reshape(128, 4, 128).astype(np.float32),
        np.broadcast_to((lam(np.arange(64), NX) * EXCHANGE)[:, None], (64, 128)).astype(np.float32),
    )


def halves(table):
    table = np.asarray(table, np.float64)
    high = table.astype(np.float32).astype(jnp.bfloat16)
    low = (table - high.astype(np.float64)).astype(np.float32).astype(jnp.bfloat16)
    return np.stack([high, low])


def split(value):
    high = value.astype(BF16)
    return high, (value - high.astype(F32)).astype(BF16)


def dot(a, b):
    return jnp.dot(a, b, preferred_element_type=F32)


def right_product(value, table, index):
    high, low = split(value)
    rows = value.shape[0]
    both = dot(jnp.concatenate([high, low], axis=0), table[index, 0])
    return both[:rows] + both[rows:] + dot(high, table[index, 1])


def left_product(table, index, value):
    high, low = split(value)
    cols = value.shape[1]
    both = dot(table[index, 0], jnp.concatenate([high, low], axis=1))
    return both[:, :cols] + both[:, cols:] + dot(table[index, 1], high)


def swap_lanes(values):
    values = list(values)
    lane = lax.broadcasted_iota(jnp.int32, values[0].shape, 1)
    step = len(values) // 2
    width = 64
    while step:
        low = (lane & width) == 0
        for i in range(len(values)):
            if i & step == 0:
                a, b = values[i], values[i + step]
                values[i] = jnp.where(low, a, pltpu.roll(b, width, 1))
                values[i + step] = jnp.where(low, pltpu.roll(a, 128 - width, 1), b)
        step //= 2
        width //= 2
    return values


PAIR = ((0, 3, 4), (3, 1, 5), (4, 5, 2))
FORWARD, BACKWARD = 0, 2
XF, XM, XB = range(3)


def transform(
    m_hbm, k_hbm, tabz_hbm, taby_hbm, tabx_hbm, lam_hbm, lamx_hbm,
    m, r6,
    kraw, tabz, tabyf, tabyb, tabx, lam, lamx, kp, k2, kq, kn_out, kn_in, kr_out, kr_in,
    r1, s2, r2, s3, r3, spec, s4, r4, s5, r5, s6,
    local_sem, send_sem, recv_sem, kn_sems,
):
    gx, gy, gz = lax.axis_index("gx"), lax.axis_index("gy"), lax.axis_index("gz")
    core, top = lax.rem(gx, 2), gx // 2
    place_xy = 2 * gy + top
    place_z = 4 * core + gz
    load_m = pltpu.make_async_copy(m_hbm, m, local_sem.at[0])
    load_m.start()

    by_y = lambda p: {"gy": p}
    on_z = [(z, {"gz": z}) for z in (lax.rem(gz + d, 4) for d in (2, 1, 3))]
    on_xy = [
        (2 * y + x, {"gx": 2 * x + core, "gy": y})
        for y, x in (
            (4 * lax.rem(gy // 4 + p, 2) + lax.rem(gy + d, 4), lax.rem(top + f, 2))
            for p, d, f in (
                (1, 2, 0), (1, 1, 0), (1, 3, 0), (1, 2, 1), (0, 2, 1), (1, 0, 0), (1, 1, 1), (1, 3, 1),
                (0, 1, 1), (0, 3, 1), (0, 2, 0), (1, 0, 1), (0, 0, 1), (0, 1, 0), (0, 3, 0),
            )
        )
    ]
    on_cz = [
        (4 * k + z, {"gx": 2 * top + k, "gz": z})
        for k, z in (
            (lax.rem(core + k, 2), lax.rem(gz + d, 4)) for d in (2, 1, 3, 0) for k in (0, 1) if (d, k) != (0, 0)
        )
    ]

    barrier = pltpu.get_barrier_semaphore()

    def repeat(start, stop, step):
        def one(j, carry):
            step(j)
            return carry

        lax.fori_loop(start, stop, one, 0)

    for _, device in on_xy + on_cz:
        pl.semaphore_signal(barrier, inc=1, device_id=device, device_id_type=MESH)
    pl.semaphore_wait(barrier, 22)

    def copy(e, n, src, dst, device):
        return pltpu.make_async_remote_copy(
            src_ref=src, dst_ref=dst, send_sem=send_sem.at[e, n], recv_sem=recv_sem.at[e, n],
            device_id=device, device_id_type=MESH,
        )

    def send_all(e, n, src, dst, me, others):
        for p, device in others:
            copy(e, n, src.at[n, p], dst.at[n, me], device).start()
        dst[n, me] = src[n, me]

    def arrived(e, n, dst, count):
        part = dst.at[n, pl.ds(0, count - 1)]
        copy(e, n, part, part, by_y(lax.rem(gy + 1, 8))).wait_recv()

    def send_both(e, c, src, dst):
        for p, device in on_cz:
            copy(e, c, src.at[c, :, p], dst.at[c, :, place_z], device).start()
        dst[c, :, place_z] = src[c, :, place_z]

    def both_arrived(e, c, dst):
        part = dst.at[c, :, pl.ds(0, 7)]
        copy(e, c, part, part, by_y(lax.rem(gy + 1, 8))).wait_recv()

    load_m.wait()
    m_blocks = m.reshape(3, 4, 4, 32, 128)

    def send_m(n):
        c, half = n // 2, lax.rem(n, 2)
        rows = pl.ds(pl.multiple_of(16 * half, 16), 16)

        for p, device in on_z:
            copy(0, n, m_blocks.at[c, p, :, rows, :], r1.at[n, gz], device).start()
        r1[n, gz] = m_blocks[c, gz, :, rows, :]

    repeat(0, 6, send_m)

    loads = [
        pltpu.make_async_copy(tabz_hbm, tabz, local_sem.at[0]),
        pltpu.make_async_copy(k_hbm, kraw, local_sem.at[1]),
        pltpu.make_async_copy(lam_hbm.at[(2 * place_z + top) * 8 + gy], lam, local_sem.at[2]),
        pltpu.make_async_copy(lamx_hbm, lamx, local_sem.at[3]),
        pltpu.make_async_copy(taby_hbm.at[0:2], tabyf, local_sem.at[4]),
        pltpu.make_async_copy(tabx_hbm, tabx, local_sem.at[5]),
        pltpu.make_async_copy(taby_hbm.at[2:4], tabyb, local_sem.at[6]),
    ]
    for load in loads:
        load.start()

    loads[1].wait()

    @pl.when(gy == 4)
    def _():
        for cc in range(6):
            for i in range(16):
                kn_out[cc, i : i + 1, 0:64] = kraw[cc, i, 0:1, :]

    kn = pltpu.make_async_remote_copy(
        src_ref=kn_out, dst_ref=kn_in, send_sem=kn_sems.at[0], recv_sem=kn_sems.at[1],
        device_id=by_y(0), device_id_type=MESH,
    )

    @pl.when(gy == 4)
    def _():
        kn.start()

    loads[0].wait()

    def z_forward(n):
        arrived(0, n, r1, 4)
        near = [r1[n, s].reshape(64, 128) for s in range(2)]
        far = [r1[n, s + 2].reshape(64, 128) for s in range(2)]
        out = [
            right_product(jnp.concatenate([a + b for a, b in zip(near, far)], axis=1), tabz, FORWARD),
            right_product(jnp.concatenate([a - b for a, b in zip(near, far)], axis=1), tabz, FORWARD + 1),
        ]
        for parity in range(2):
            for t in range(2):
                parts = swap_lanes(
                    [out[parity][16 * x : 16 * x + 16, 128 * t : 128 * t + 128] for x in range(4)]
                )
                for q in range(4):
                    s2[n, 2 * (4 * t + q) + parity] = parts[q]
        send_all(1, n, s2, r2_blocks, place_xy, on_xy)

    r2_blocks = r2.reshape(6, 16, 16, 128)
    s5_blocks = s5.reshape(6, 16, 16, 128)
    repeat(0, 3, z_forward)

    late = gy >= 4
    first = gy == 0
    middle = first & (place_z == 0)

    @pl.when(first)
    def _():
        kn.wait_recv()

    for load in loads[2:4]:
        load.wait()

    def prepare(cc):
        for v in range(2):
            own, other = [], []
            for g in range(8):
                i = 8 * v + g
                even = kraw[cc, i, pl.ds(0, 16, stride=2), :]
                even = jnp.where(late, kraw[cc, i, pl.ds(2, 16, stride=2), :], even)
                odd = kraw[cc, i, pl.ds(1, 16, stride=2), :]
                row = lax.broadcasted_iota(jnp.int32, even.shape, 0)
                nyquist = jnp.broadcast_to(kn_in[cc, i : i + 1, 0:64], even.shape)
                nyquist = jnp.where(first, nyquist, even)
                packed = jnp.where(top == 1, nyquist, even)
                if i == 0:
                    packed = jnp.where(middle, 0.5 * (even + nyquist), packed)
                    kr_out[cc, 0:1, 0:64] = 0.5 * (even - nyquist)[0:1, :]
                even = jnp.where(row == 0, packed, even)
                own.append(jnp.where(top == 1, odd, even))
                other.append(jnp.where(top == 1, even, odd))
            kp[cc, 2 * top + v] = -INVERSE_COUNT * jnp.concatenate(own, axis=0).T
            kq[cc, v] = -INVERSE_COUNT * jnp.concatenate(other, axis=0).T

    repeat(0, 6, prepare)
    repeat(3, 6, z_forward)

    across = {"gx": lax.rem(gx + 2, 4)}
    shares = [
        pltpu.make_async_remote_copy(
            src_ref=src, dst_ref=dst, send_sem=kn_sems.at[n], recv_sem=kn_sems.at[n + 1],
            device_id=across, device_id_type=MESH,
        )
        for n, src, dst in ((2, kq, kp.at[:, pl.ds(2 * top, 2)]), (4, kr_out, kr_in))
    ]
    for share in shares:
        share.start()

    for load in loads[4:]:
        load.wait()
    row = lax.broadcasted_iota(jnp.int32, (128, 128), 0)
    lane = lax.broadcasted_iota(jnp.int32, (128, 128), 1)
    real = (lane & 16) == 0
    packed_lane = first & (top == 0) & ((lane & 15) == 0)
    low = (row & 2) == 0
    lone = ((row & 125) == 0, row < 0)
    partner = lambda z: jnp.where(real, pltpu.roll(z, 112, 1), pltpu.roll(z, 16, 1))

    def y_forward(c):
        arrived(1, 2 * c, r2_blocks, 16)
        arrived(1, 2 * c + 1, r2_blocks, 16)
        part = lambda h, x: r2[pl.ds(2 * c, 2), 4 * h : 4 * h + 4, x].reshape(128, 128)
        halves_x = []
        for h in range(2):
            a, b = part(h, 0), part(h, 1)
            halves_x.append(jnp.concatenate([a + b, a - b], axis=1))
        out = [[], []]
        for parity, value in enumerate((halves_x[0] + halves_x[1], halves_x[0] - halves_x[1])):
            rows = left_product(tabyf, parity, value)
            for e in range(2):
                cosine, sine = rows[:128, 128 * e : 128 * e + 128], rows[128:, 128 * e : 128 * e + 128]
                turned = partner(sine)
                plain = cosine + jnp.where(real, turned, -turned)
                single = jnp.where(
                    low, jnp.where(real, cosine, -turned), jnp.where(real, partner(cosine), -sine)
                )
                out[e].append(jnp.where(packed_lane & ~lone[parity], single, plain))
        for e in range(2):
            parts = swap_lanes([out[e][g % 2][32 * (g // 2) : 32 * (g // 2) + 32] for g in range(8)])
            for x in range(8):
                s3[c, e, pl.ds(x, 32, stride=8), :] = parts[x]
        send_both(2, c, s3_blocks, r3)

    s3_blocks = s3.reshape(3, 2, 8, 32, 128)
    r4_blocks = r4.reshape(3, 2, 8, 32, 128)
    repeat(0, 3, y_forward)

    def x_forward(c):
        both_arrived(2, c, r3)
        tiles = [r3[c, :, :, 8 * v : 8 * v + 8, :].reshape(128, 128) for v in range(4)]
        for v in range(4):
            spec[c, v] = left_product(tabx, XF, tiles[v])
        for j in range(2):
            spec[c, 4 + j] = left_product(tabx, XM, tiles[2 * j])

    repeat(0, 2, x_forward)

    for share in shares:
        share.wait_recv()
    corner_lane = middle & (top == 0) & (lax.broadcasted_iota(jnp.int32, (64, 128), 1) == 0)
    for cc in range(6):
        for j, source in enumerate((kr_out, kr_in)):
            column = jnp.broadcast_to(source[cc, 0:1, 0:64], (128, 64)).T
            column = -INVERSE_COUNT * column + (2.0 * EXCHANGE * INVERSE_COUNT if cc < 3 else 0.0)
            k2[cc, j] = jnp.where(corner_lane, column, 0.0)
        if cc < 3:
            for v in range(4):
                kp[cc, v] += INVERSE_COUNT * (lamx[...] + lam[v : v + 1, :])
    x_forward(2)

    for c in range(3):
        for v in range(4):
            terms = []
            for part in range(2):
                rows = slice(64 * part, 64 * part + 64)
                total = sum(kp[PAIR[c][d], v] * spec[d, v, rows, :] for d in range(3))
                if v % 2 == 0:
                    total = total + sum(
                        k2[PAIR[c][d], v // 2] * spec[d, 4 + v // 2, rows, :] for d in range(3)
                    )
                terms.append(total)
            out = left_product(tabx, XB, jnp.concatenate(terms, axis=0))
            s4[c, :, :, 8 * v : 8 * v + 8, :] = out.reshape(2, 8, 8, 128)
        send_both(3, c, s4, r4_blocks)

    alternate = (1 - 2 * (row & 1)).astype(F32)

    def y_backward(c):
        both_arrived(3, c, r4_blocks)
        pieces = [swap_lanes([r4[c, e, pl.ds(x, 32, stride=8), :] for x in range(8)]) for e in range(2)]
        out = [[], []]
        for parity in range(2):
            value = [
                jnp.concatenate([pieces[e][2 * g + parity] for g in range(4)], axis=0) for e in range(2)
            ]
            masked = [jnp.where(low & ~lone[parity], z, 0.0) for z in value]
            rows = left_product(tabyb, parity, jnp.concatenate(value, axis=1))
            rows_low = left_product(tabyb, parity, jnp.concatenate(masked, axis=1))
            for e in range(2):
                cols = slice(128 * e, 128 * e + 128)
                cosine, sine = rows[:128, cols], rows[128:, cols]
                cosine_low, sine_low = rows_low[:128, cols], rows_low[128:, cols]
                turned = partner(sine)
                plain = cosine + jnp.where(real, -turned, turned)
                cosine_high, sine_high = cosine - cosine_low, sine - sine_low
                base = 0.0
                if parity == 0:
                    base = value[e][0:1, :] + alternate * value[e][2:3, :]
                    cosine_high = cosine_high - base
                double = jnp.where(real, cosine_low - partner(sine_low), partner(cosine_high) - sine_high)
                out[e].append(jnp.where(packed_lane, 2.0 * double + base, plain))
        for h in range(2):
            even, odd = [out[e][0] + out[e][1] if h == 0 else out[e][0] - out[e][1] for e in range(2)]
            for x, value in enumerate((even + odd, even - odd)):
                s5[pl.ds(2 * c, 2), 4 * h : 4 * h + 4, x] = value.reshape(2, 4, 16, 128)
        send_all(4, 2 * c, s5_blocks, r5, place_xy, on_xy)
        send_all(4, 2 * c + 1, s5_blocks, r5, place_xy, on_xy)

    repeat(0, 3, y_backward)

    def z_backward(n):
        arrived(4, n, r5, 16)
        tiles = [[], []]
        for parity in range(2):
            for t in range(2):
                parts = swap_lanes([r5[n, 2 * (4 * t + q) + parity] for q in range(4)])
                tiles[parity].append(jnp.concatenate(parts, axis=0))
        out = [right_product(jnp.concatenate(tiles[p], axis=1), tabz, BACKWARD + p) for p in range(2)]
        for h, value in enumerate((out[0] + out[1], out[0] - out[1])):
            s6[n, 2 * h] = value[:, 0:128]
            s6[n, 2 * h + 1] = value[:, 128:256]
        send_all(5, n, s6, r6, gz, on_z)

    repeat(0, 6, z_backward)

    def sent(e, chunks, part):
        repeat(0, chunks, lambda n: copy(e, n, part(n), part(n), by_y(lax.rem(gy + 1, 8))).wait_send())

    sent(0, 6, lambda n: r1.at[n, pl.ds(0, 3)])
    sent(1, 6, lambda n: s2.at[n, pl.ds(0, 15)])
    sent(2, 3, lambda n: s3_blocks.at[n, :, pl.ds(0, 7)])
    sent(3, 3, lambda n: s4.at[n, :, pl.ds(0, 7)])
    sent(4, 6, lambda n: s5_blocks.at[n, pl.ds(0, 15)])
    for share in shares:
        share.wait_send()

    @pl.when(gy == 4)
    def _():
        kn.wait_send()

    repeat(0, 6, lambda n: arrived(5, n, r6, 4))
    sent(5, 6, lambda n: s6.at[n, pl.ds(0, 3)])


def advance(m, demag, applied, pred_hbm, torque_hbm, pout, tout, sems):
    cross = lambda a, b: [
        a[1] * b[2] - a[2] * b[1],
        a[2] * b[0] - a[0] * b[2],
        a[0] * b[1] - a[1] * b[0],
    ]
    stores = []
    for s in range(4):
        planes = slice(4 * s, 4 * s + 4)
        for half in range(2):
            rows = slice(16 * half, 16 * half + 16)
            mag = [m[c, planes, rows, :] for c in range(3)]
            field = [demag[2 * c + half, s].reshape(4, 16, 128) + applied[c] for c in range(3)]
            precess = cross(mag, field)
            twist = cross(mag, precess)
            torque = [-(precess[c] + DAMPING * twist[c]) / (1.0 + DAMPING * DAMPING) for c in range(3)]
            stepped = [mag[c] + STEP * torque[c] for c in range(3)]
            length = jnp.sqrt(stepped[0] * stepped[0] + stepped[1] * stepped[1] + stepped[2] * stepped[2])
            for c in range(3):
                tout[c, planes, rows, :] = torque[c]
                pout[c, planes, rows, :] = stepped[c] / length
        stores += [
            pltpu.make_async_copy(tout.at[:, planes], torque_hbm.at[:, planes], sems.at[s, 0]),
            pltpu.make_async_copy(pout.at[:, planes], pred_hbm.at[:, planes], sems.at[s, 1]),
        ]
        stores[-2].start()
        stores[-1].start()
    for store in stores:
        store.wait()


def shards(magnetization, kernel, applied):
    zf, zb = z_tables()
    yf, yb = y_tables()
    tabz = np.stack([halves(t) for t in zf + zb])
    taby = np.stack([halves(t) for t in yf + yb])
    tabx = np.stack([halves(t) for t in x_tables()])
    lam, lamx = eigen_tables()
    shape = magnetization.shape
    anywhere = pl.BlockSpec(memory_space=pltpu.HBM)
    in_vmem = pl.BlockSpec(memory_space=pltpu.VMEM)
    vmem = lambda *shape, dtype=F32: pltpu.VMEM(shape, dtype)
    m, demag = pl.pallas_call(
        transform,
        out_shape=[vmem(*shape), vmem(6, 4, 64, 128)],
        in_specs=[anywhere] * 7,
        out_specs=[in_vmem, in_vmem],
        scratch_shapes=[
            vmem(6, 16, 64, 64),
            vmem(4, 2, 256, 256, dtype=BF16),
            vmem(2, 2, 256, 128, dtype=BF16),
            vmem(2, 2, 256, 128, dtype=BF16),
            vmem(3, 2, 128, 128, dtype=BF16),
            vmem(4, 128),
            vmem(64, 128),
            vmem(6, 4, 64, 128),
            vmem(6, 2, 64, 128),
            vmem(6, 2, 64, 128),
            vmem(6, 16, 128),
            vmem(6, 16, 128),
            vmem(6, 8, 128),
            vmem(6, 8, 128),
            vmem(6, 4, 4, 16, 128),
            vmem(6, 16, 16, 128),
            vmem(6, 8, 2, 16, 128),
            vmem(3, 2, 256, 128),
            vmem(3, 2, 8, 32, 128),
            vmem(3, 6, 128, 128),
            vmem(3, 2, 8, 32, 128),
            vmem(3, 2, 256, 128),
            vmem(6, 8, 2, 16, 128),
            vmem(6, 16, 16, 128),
            vmem(6, 4, 64, 128),
            pltpu.SemaphoreType.DMA((7,)),
            pltpu.SemaphoreType.DMA((6, 6)),
            pltpu.SemaphoreType.DMA((6, 6)),
            pltpu.SemaphoreType.DMA((6,)),
        ],
        compiler_params=pltpu.CompilerParams(
            collective_id=0, has_side_effects=True, vmem_limit_bytes=62 * 1024 * 1024
        ),
    )(
        magnetization, kernel, jnp.asarray(tabz), jnp.asarray(taby), jnp.asarray(tabx),
        jnp.asarray(lam), jnp.asarray(lamx),
    )
    return pl.pallas_call(
        advance,
        out_shape=[jax.ShapeDtypeStruct(shape, F32)] * 2,
        in_specs=[in_vmem, in_vmem, pl.BlockSpec(memory_space=pltpu.SMEM)],
        out_specs=[anywhere] * 2,
        scratch_shapes=[vmem(*shape), vmem(*shape), pltpu.SemaphoreType.DMA((4, 2))],
        compiler_params=pltpu.CompilerParams(vmem_limit_bytes=16 * 1024 * 1024),
    )(m, demag, applied)


def solution(mesh):
    return jax.shard_map(
        shards,
        mesh=mesh,
        in_specs=(P(None, "gx", "gy", "gz"), P(None, ("gx", "gz"), "gy", None), P()),
        out_specs=(P(None, "gx", "gy", "gz"), P(None, "gx", "gy", "gz")),
        check_vma=False,
    )
```

```python
import math

import jax
import jax.numpy as jnp
import numpy as np
from jax import lax
from jax.experimental import pallas as pl
from jax.experimental.pallas import tpu as pltpu
from jax.sharding import PartitionSpec as P

MESH = pl.DeviceIdType.MESH
F32 = jnp.float32
BF16 = jnp.bfloat16
NX, NY, NZ = 64, 256, 512
EXCHANGE = 1.0
DAMPING = 0.3
STEP = 0.2
INVERSE_COUNT = 1.0 / (NX * NY * NZ)


def wave_z(block, slot):
    odd = slot >= 16
    return 64 * block + 2 * (slot % 16) + np.where(odd, 1, np.where(block >= 4, 2, 0))


def turn(rows, cols, length):
    angle = 2.0 * np.pi / length * ((rows[:, None] * cols[None, :]) % length)
    return np.cos(angle), np.sin(angle)


def grid(*counts):
    return [a.reshape(-1) for a in np.meshgrid(*(np.arange(n) for n in counts), indexing="ij")]


def z_tables():
    forward, backward = [], []
    for parity in range(2):
        block, part, slot = grid(8, 2, 16)
        cosine, sine = turn(np.arange(NZ // 2), wave_z(block, slot + 16 * parity), NZ)
        table = np.where(part == 0, cosine, -sine)
        weight = np.full(256, 2.0)
        if parity == 0:
            packed = (block == 0) & (slot == 0)
            alternate = 1.0 - 2.0 * (np.arange(NZ // 2) % 2)
            table[:, packed & (part == 1)] = alternate[:, None]
            weight[packed] = 1.0
        forward.append(table)
        backward.append(weight[:, None] * table.T)
    return forward, backward


def wave_y(owner, tile, group):
    return 128 * (tile // 2) + 16 * owner + 8 * (tile % 2) + group


def y_tables():
    forward, backward = [], []
    for parity in range(2):
        group, owner, tile = grid(4, 8, 4)
        half, block, row = grid(2, 4, 16)
        tables = turn(wave_y(owner, tile, 2 * group + parity), 32 * block + 16 * half + row, NY)
        forward.append(np.concatenate(tables, axis=0))
        backward.append(np.concatenate([t.T for t in tables], axis=0))
    return forward, backward


def x_tables():
    part, kx = grid(2, 64)
    parity, owner, xs, xp = grid(2, 8, 4, 2)
    cosine, sine = turn(kx, 4 * owner + xs, NX)
    out_re, in_re = (part == 0)[:, None], (xp == 0)[None, :]
    mine = kx[:, None] % 2 == parity[None, :]
    forward = np.where(mine, np.where(out_re == in_re, cosine, np.where(out_re, sine, -sine)), 0.0)
    mirrored = np.where(in_re, forward, -forward)
    backward = np.where(mine, np.where(out_re == in_re, cosine, np.where(in_re, -sine, sine)), 0.0).T
    return forward, mirrored, backward


def eigen_tables():
    lam = lambda k, n: 2.0 * np.cos(2.0 * np.pi * k / n) - 2.0
    owner, parity, block, tile, group, slot = grid(8, 2, 8, 4, 8, 16)
    ky, kz = wave_y(owner, tile, group), wave_z(block, slot + 16 * parity)
    z_part = lam(kz, NZ)
    packed = (block == 0) & (parity == 0) & (slot == 0)
    z_part = np.where(packed, np.where(ky % 128 == 0, -2.0, np.where(ky > 128, -4.0, 0.0)), z_part)
    table = (lam(ky, NY) + z_part) * EXCHANGE
    return (
        table.reshape(128, 4, 128).astype(np.float32),
        np.broadcast_to((lam(np.arange(64), NX) * EXCHANGE)[:, None], (64, 128)).astype(np.float32),
    )


def halves(table):
    table = np.asarray(table, np.float64)
    high = table.astype(np.float32).astype(jnp.bfloat16)
    low = (table - high.astype(np.float64)).astype(np.float32).astype(jnp.bfloat16)
    return np.stack([high, low])


def left_halves(table):
    high, low = halves(table)
    return np.concatenate([high, high, low], axis=1)


def split(value):
    high = value.astype(BF16)
    return high, (value - high.astype(F32)).astype(BF16)


def dot(a, b):
    return jnp.dot(a, b, preferred_element_type=F32)


def right_product(value, table, index):
    high, low = split(value)
    rows = value.shape[0]
    both = dot(jnp.concatenate([high, low], axis=0), table[index, 0])
    return both[:rows] + both[rows:] + dot(high, table[index, 1])


def left_product(table, index, value):
    high, low = split(value)
    return dot(table[index], jnp.concatenate([high, low, high], axis=0))


def wide_product(table, index, value):
    high, low = split(value)
    cols = value.shape[1]
    both = dot(table[index, 0], jnp.concatenate([high, low], axis=1))
    return both[:, :cols] + both[:, cols:] + dot(table[index, 1], high)


def swap_lanes(values):
    values = list(values)
    lane = lax.broadcasted_iota(jnp.int32, values[0].shape, 1)
    step = len(values) // 2
    width = 64
    while step:
        low = (lane & width) == 0
        for i in range(len(values)):
            if i & step == 0:
                a, b = values[i], values[i + step]
                values[i] = jnp.where(low, a, pltpu.roll(b, width, 1))
                values[i + step] = jnp.where(low, pltpu.roll(a, 128 - width, 1), b)
        step //= 2
        width //= 2
    return values


PAIR = ((0, 3, 4), (3, 1, 5), (4, 5, 2))
FORWARD, BACKWARD = 0, 2
XF, XM, XB = range(3)


def transform(
    m_hbm, k_hbm, tabz_hbm, taby_hbm, tabx_hbm, lam_hbm, lamx_hbm,
    m, r6,
    kraw, tabz, tabyf, tabyb, tabx, lam, lamx, kp, k2, kq, kn_out, kn_in,
    r1, s2, r2, s3, r3, spec, s4, r4, s5, r5, s6,
    local_sem, send_sem, recv_sem, kn_sems,
):
    gx, gy, gz = lax.axis_index("gx"), lax.axis_index("gy"), lax.axis_index("gz")
    core, top = lax.rem(gx, 2), gx // 2
    place_xy = 2 * gy + top
    place_z = 4 * core + gz
    load_m = pltpu.make_async_copy(m_hbm, m, local_sem.at[0])
    load_m.start()
    load_k = pltpu.make_async_copy(k_hbm, kraw, local_sem.at[1])
    load_k.start()

    by_y = lambda p: {"gy": p}
    on_z = [(z, {"gz": z}) for z in (lax.rem(gz + d, 4) for d in (2, 1, 3))]
    on_xy = [
        (2 * y + x, {"gx": 2 * x + core, "gy": y})
        for y, x in (
            (4 * lax.rem(gy // 4 + p, 2) + lax.rem(gy + d, 4), lax.rem(top + f, 2))
            for p, d, f in (
                (1, 2, 0), (1, 1, 0), (1, 3, 0), (1, 2, 1), (0, 2, 1), (1, 0, 0), (1, 1, 1), (1, 3, 1),
                (0, 1, 1), (0, 3, 1), (0, 2, 0), (1, 0, 1), (0, 0, 1), (0, 1, 0), (0, 3, 0),
            )
        )
    ]
    on_cz = [
        (4 * k + z, {"gx": 2 * top + k, "gz": z})
        for k, z in (
            (lax.rem(core + k, 2), lax.rem(gz + d, 4)) for d in (2, 1, 3, 0) for k in (0, 1) if (d, k) != (0, 0)
        )
    ]

    barrier = pltpu.get_barrier_semaphore()

    def repeat(start, stop, step):
        def one(j, carry):
            step(j)
            return carry

        lax.fori_loop(start, stop, one, 0)

    for _, device in on_xy + on_cz:
        pl.semaphore_signal(barrier, inc=1, device_id=device, device_id_type=MESH)
    pl.semaphore_wait(barrier, 22)

    def copy(e, n, src, dst, device):
        return pltpu.make_async_remote_copy(
            src_ref=src, dst_ref=dst, send_sem=send_sem.at[e, n], recv_sem=recv_sem.at[e, n],
            device_id=device, device_id_type=MESH,
        )

    def send_all(e, n, src, dst, me, others):
        for p, device in others:
            copy(e, n, src.at[n, p], dst.at[n, me], device).start()
        dst[n, me] = src[n, me]

    def arrived(e, n, dst, count):
        part = dst.at[n, pl.ds(0, count - 1)]
        copy(e, n, part, part, by_y(lax.rem(gy + 1, 8))).wait_recv()

    def send_both(e, c, src, dst):
        for p, device in on_cz:
            copy(e, c, src.at[c, :, p], dst.at[c, :, place_z], device).start()
        dst[c, :, place_z] = src[c, :, place_z]

    def both_arrived(e, c, dst):
        part = dst.at[c, :, pl.ds(0, 7)]
        copy(e, c, part, part, by_y(lax.rem(gy + 1, 8))).wait_recv()

    load_m.wait()
    m_blocks = m.reshape(3, 4, 4, 32, 128)

    def send_m(n):
        c, half = n // 2, lax.rem(n, 2)
        rows = pl.ds(pl.multiple_of(16 * half, 16), 16)

        for p, device in on_z:
            copy(0, n, m_blocks.at[c, p, :, rows, :], r1.at[n, gz], device).start()
        r1[n, gz] = m_blocks[c, gz, :, rows, :]

    repeat(0, 6, send_m)

    loads = [
        pltpu.make_async_copy(tabz_hbm, tabz, local_sem.at[0]),
        pltpu.make_async_copy(lam_hbm.at[(2 * place_z + top) * 8 + gy], lam, local_sem.at[2]),
        pltpu.make_async_copy(lamx_hbm, lamx, local_sem.at[3]),
        pltpu.make_async_copy(taby_hbm.at[0:2], tabyf, local_sem.at[4]),
        pltpu.make_async_copy(tabx_hbm, tabx, local_sem.at[5]),
        pltpu.make_async_copy(taby_hbm.at[2:4], tabyb, local_sem.at[6]),
    ]
    for load in loads:
        load.start()

    load_k.wait()
    late = gy >= 4
    first = gy == 0

    def prepare(cc):
        for v in range(2):
            own, other = [], []
            for g in range(8):
                i = 8 * v + g
                even = kraw[cc, i, pl.ds(0, 16, stride=2), :]
                even = jnp.where(late, kraw[cc, i, pl.ds(2, 16, stride=2), :], even)
                odd = kraw[cc, i, pl.ds(1, 16, stride=2), :]
                own.append(jnp.where(top == 1, odd, even))
                other.append(jnp.where(top == 1, even, odd))
            kp[cc, 2 * top + v] = -INVERSE_COUNT * jnp.concatenate(own, axis=0).T
            kq[cc, v] = -INVERSE_COUNT * jnp.concatenate(other, axis=0).T

    def share(n, start, count):
        part = pl.ds(start, count)
        return pltpu.make_async_remote_copy(
            src_ref=kq.at[part], dst_ref=kp.at[part, pl.ds(2 * top, 2)],
            send_sem=kn_sems.at[n], recv_sem=kn_sems.at[n + 1],
            device_id={"gx": lax.rem(gx + 2, 4)}, device_id_type=MESH,
        )

    shares = [share(0, 0, 2), share(2, 2, 4)]
    repeat(0, 2, prepare)
    shares[0].start()

    def nyquist(n):
        return pltpu.make_async_remote_copy(
            src_ref=kn_out, dst_ref=kn_in.at[n], send_sem=kn_sems.at[4], recv_sem=kn_sems.at[5 + n],
            device_id={"gx": core, "gy": 0}, device_id_type=MESH,
        )

    @pl.when(gy == 4)
    def _():
        for cc in range(6):
            for i in range(16):
                kn_out[cc, i : i + 1, 0:64] = kraw[cc, i, 0:1, :]
        nyquist(top).start()

    repeat(2, 6, prepare)
    loads[0].wait()

    def z_forward(n):
        arrived(0, n, r1, 4)
        near = [r1[n, s].reshape(64, 128) for s in range(2)]
        far = [r1[n, s + 2].reshape(64, 128) for s in range(2)]
        out = [
            right_product(jnp.concatenate([a + b for a, b in zip(near, far)], axis=1), tabz, FORWARD),
            right_product(jnp.concatenate([a - b for a, b in zip(near, far)], axis=1), tabz, FORWARD + 1),
        ]
        for parity in range(2):
            for t in range(2):
                parts = swap_lanes(
                    [out[parity][16 * x : 16 * x + 16, 128 * t : 128 * t + 128] for x in range(4)]
                )
                for q in range(4):
                    s2[n, 2 * (4 * t + q) + parity] = parts[q]
        send_all(1, n, s2, r2_blocks, place_xy, on_xy)

    r2_blocks = r2.reshape(6, 16, 16, 128)
    s5_blocks = s5.reshape(6, 16, 16, 128)
    repeat(0, 6, z_forward)
    shares[1].start()

    for load in loads[1:]:
        load.wait()
    row = lax.broadcasted_iota(jnp.int32, (128, 128), 0)
    lane = lax.broadcasted_iota(jnp.int32, (128, 128), 1)
    real = (lane & 16) == 0
    packed_lane = first & (top == 0) & ((lane & 15) == 0)
    low = (row & 2) == 0
    lone = ((row & 125) == 0, row < 0)
    from_imag = lambda z: pltpu.roll(z, 112, 1)
    from_real = lambda z: pltpu.roll(z, 16, 1)
    partner = lambda z: jnp.where(real, from_imag(z), from_real(z))

    def y_forward(c):
        arrived(1, 2 * c, r2_blocks, 16)
        arrived(1, 2 * c + 1, r2_blocks, 16)
        part = lambda h, x: r2[pl.ds(2 * c, 2), 4 * h : 4 * h + 4, x].reshape(128, 128)
        halves_x = []
        for h in range(2):
            a, b = part(h, 0), part(h, 1)
            halves_x.append(jnp.concatenate([a + b, a - b], axis=1))
        out = [[], []]
        for parity, value in enumerate((halves_x[0] + halves_x[1], halves_x[0] - halves_x[1])):
            rows = wide_product(tabyf, parity, value)
            for e in range(2):
                cosine, sine = rows[:128, 128 * e : 128 * e + 128], rows[128:, 128 * e : 128 * e + 128]
                turned = partner(sine)
                plain = cosine + jnp.where(real, turned, -turned)
                single = jnp.where(
                    low, jnp.where(real, cosine, -turned), jnp.where(real, from_imag(cosine), -sine)
                )
                out[e].append(jnp.where(packed_lane & ~lone[parity], single, plain))
        for e in range(2):
            parts = swap_lanes([out[e][g % 2][32 * (g // 2) : 32 * (g // 2) + 32] for g in range(8)])
            for x in range(8):
                s3[c, e, pl.ds(x, 32, stride=8), :] = parts[x]
        send_both(2, c, s3_blocks, r3)

    s3_blocks = s3.reshape(3, 2, 8, 32, 128)
    r4_blocks = r4.reshape(3, 2, 8, 32, 128)
    repeat(0, 3, y_forward)

    def x_forward(c):
        both_arrived(2, c, r3)
        tiles = [r3[c, :, :, 8 * v : 8 * v + 8, :].reshape(128, 128) for v in range(4)]
        out = left_product(tabx, XF, jnp.concatenate(tiles, axis=1))
        for v in range(4):
            spec[c, v] = out[:, 128 * v : 128 * v + 128]
        out = left_product(tabx, XM, jnp.concatenate(tiles[::2], axis=1))
        for j in range(2):
            spec[c, 4 + j] = out[:, 128 * j : 128 * j + 128]

    repeat(0, 2, x_forward)

    for piece in shares:
        piece.wait_recv()
    k2[...] = jnp.zeros_like(k2)

    @pl.when(first & (top == 0))
    def _():
        for n in range(2):
            nyquist(n).wait_recv()
        small_lane = lax.broadcasted_iota(jnp.int32, (64, 128), 1)
        corner_lane = (place_z == 0) & (small_lane == 0)

        def mend(cc):
            for v in range(4):
                rows = [
                    jnp.broadcast_to(kn_in[v // 2, cc, i : i + 1, 0:64], (16, 64))
                    for i in range(8 * (v % 2), 8 * (v % 2) + 8)
                ]
                edge = -INVERSE_COUNT * jnp.concatenate(rows, axis=0).T
                plain = kp[cc, v]
                value = jnp.where((small_lane & 15) == 0, edge, plain) if v >= 2 else plain
                if v % 2 == 0:
                    value = jnp.where(corner_lane, 0.5 * (plain + edge), value)
                    term = jnp.where(cc < 3, 2.0 * EXCHANGE * INVERSE_COUNT, 0.0)
                    k2[cc, v // 2] = jnp.where(corner_lane, 0.5 * (plain - edge) + term, 0.0)
                kp[cc, v] = value

        repeat(0, 6, mend)

    for cc in range(3):
        for v in range(4):
            kp[cc, v] += INVERSE_COUNT * (lamx[...] + lam[v : v + 1, :])
    x_forward(2)

    for c in range(3):
        tiles = []
        for v in range(4):
            terms = []
            for part in range(2):
                rows = slice(64 * part, 64 * part + 64)
                total = sum(kp[PAIR[c][d], v] * spec[d, v, rows, :] for d in range(3))
                if v % 2 == 0:
                    total = total + sum(
                        k2[PAIR[c][d], v // 2] * spec[d, 4 + v // 2, rows, :] for d in range(3)
                    )
                terms.append(total)
            tiles.append(jnp.concatenate(terms, axis=0))
        out = left_product(tabx, XB, jnp.concatenate(tiles, axis=1))
        for v in range(4):
            s4[c, :, :, 8 * v : 8 * v + 8, :] = out[:, 128 * v : 128 * v + 128].reshape(2, 8, 8, 128)
        send_both(3, c, s4, r4_blocks)

    alternate = (1 - 2 * (row & 1)).astype(F32)

    def y_backward(c):
        both_arrived(3, c, r4_blocks)
        pieces = [swap_lanes([r4[c, e, pl.ds(x, 32, stride=8), :] for x in range(8)]) for e in range(2)]
        out = [[], []]
        for parity in range(2):
            value = [
                jnp.concatenate([pieces[e][2 * g + parity] for g in range(4)], axis=0) for e in range(2)
            ]
            masked = jnp.concatenate([jnp.where(low & ~lone[parity], z, 0.0) for z in value], axis=1)
            rows = wide_product(tabyb, parity, jnp.concatenate(value, axis=1))
            rows_low = wide_product(tabyb, parity, masked)
            for e in range(2):
                cols = slice(128 * e, 128 * e + 128)
                cosine, sine = rows[:128, cols], rows[128:, cols]
                cosine_low, sine_low = rows_low[:128, cols], rows_low[128:, cols]
                turned = partner(sine)
                plain = cosine + jnp.where(real, -turned, turned)
                cosine_high, sine_high = cosine - cosine_low, sine - sine_low
                base = 0.0
                if parity == 0:
                    base = value[e][0:1, :] + alternate * value[e][2:3, :]
                    cosine_high = cosine_high - base
                double = jnp.where(real, cosine_low - from_imag(sine_low), from_real(cosine_high) - sine_high)
                out[e].append(jnp.where(packed_lane, 2.0 * double + base, plain))
        for h in range(2):
            even, odd = [out[e][0] + out[e][1] if h == 0 else out[e][0] - out[e][1] for e in range(2)]
            for x, value in enumerate((even + odd, even - odd)):
                s5[pl.ds(2 * c, 2), 4 * h : 4 * h + 4, x] = value.reshape(2, 4, 16, 128)
        send_all(4, 2 * c, s5_blocks, r5, place_xy, on_xy)
        send_all(4, 2 * c + 1, s5_blocks, r5, place_xy, on_xy)

    repeat(0, 3, y_backward)

    def z_backward(n):
        arrived(4, n, r5, 16)
        tiles = [[], []]
        for parity in range(2):
            for t in range(2):
                parts = swap_lanes([r5[n, 2 * (4 * t + q) + parity] for q in range(4)])
                tiles[parity].append(jnp.concatenate(parts, axis=0))
        out = [right_product(jnp.concatenate(tiles[p], axis=1), tabz, BACKWARD + p) for p in range(2)]
        for h, value in enumerate((out[0] + out[1], out[0] - out[1])):
            s6[n, 2 * h] = value[:, 0:128]
            s6[n, 2 * h + 1] = value[:, 128:256]
        send_all(5, n, s6, r6, gz, on_z)

    repeat(0, 6, z_backward)

    def sent(e, chunks, part):
        repeat(0, chunks, lambda n: copy(e, n, part(n), part(n), by_y(lax.rem(gy + 1, 8))).wait_send())

    sent(0, 6, lambda n: r1.at[n, pl.ds(0, 3)])
    sent(1, 6, lambda n: s2.at[n, pl.ds(0, 15)])
    sent(2, 3, lambda n: s3_blocks.at[n, :, pl.ds(0, 7)])
    sent(3, 3, lambda n: s4.at[n, :, pl.ds(0, 7)])
    sent(4, 6, lambda n: s5_blocks.at[n, pl.ds(0, 15)])
    for piece in shares:
        piece.wait_send()

    @pl.when(gy == 4)
    def _():
        nyquist(top).wait_send()

    repeat(0, 6, lambda n: arrived(5, n, r6, 4))
    sent(5, 6, lambda n: s6.at[n, pl.ds(0, 3)])


def advance(m, demag, applied, pred_hbm, torque_hbm, pout, tout, sems):
    cross = lambda a, b: [
        a[1] * b[2] - a[2] * b[1],
        a[2] * b[0] - a[0] * b[2],
        a[0] * b[1] - a[1] * b[0],
    ]
    stores = []
    for s in range(4):
        planes = slice(4 * s, 4 * s + 4)
        for half in range(2):
            rows = slice(16 * half, 16 * half + 16)
            mag = [m[c, planes, rows, :] for c in range(3)]
            field = [demag[2 * c + half, s].reshape(4, 16, 128) + applied[c] for c in range(3)]
            precess = cross(mag, field)
            twist = cross(mag, precess)
            torque = [-(precess[c] + DAMPING * twist[c]) / (1.0 + DAMPING * DAMPING) for c in range(3)]
            stepped = [mag[c] + STEP * torque[c] for c in range(3)]
            length = jnp.sqrt(stepped[0] * stepped[0] + stepped[1] * stepped[1] + stepped[2] * stepped[2])
            for c in range(3):
                tout[c, planes, rows, :] = torque[c]
                pout[c, planes, rows, :] = stepped[c] / length
        stores += [
            pltpu.make_async_copy(tout.at[:, planes], torque_hbm.at[:, planes], sems.at[s, 0]),
            pltpu.make_async_copy(pout.at[:, planes], pred_hbm.at[:, planes], sems.at[s, 1]),
        ]
        stores[-2].start()
        stores[-1].start()
    for store in stores:
        store.wait()


def shards(magnetization, kernel, applied):
    zf, zb = z_tables()
    yf, yb = y_tables()
    tabz = np.stack([halves(t) for t in zf + zb])
    taby = np.stack([halves(t) for t in yf + yb])
    tabx = np.stack([left_halves(t) for t in x_tables()])
    lam, lamx = eigen_tables()
    shape = magnetization.shape
    anywhere = pl.BlockSpec(memory_space=pltpu.HBM)
    in_vmem = pl.BlockSpec(memory_space=pltpu.VMEM)
    vmem = lambda *shape, dtype=F32: pltpu.VMEM(shape, dtype)
    m, demag = pl.pallas_call(
        transform,
        out_shape=[vmem(*shape), vmem(6, 4, 64, 128)],
        in_specs=[anywhere] * 7,
        out_specs=[in_vmem, in_vmem],
        scratch_shapes=[
            vmem(6, 16, 64, 64),
            vmem(4, 2, 256, 256, dtype=BF16),
            vmem(2, 2, 256, 128, dtype=BF16),
            vmem(2, 2, 256, 128, dtype=BF16),
            vmem(3, 128, 384, dtype=BF16),
            vmem(4, 128),
            vmem(64, 128),
            vmem(6, 4, 64, 128),
            vmem(6, 2, 64, 128),
            vmem(6, 2, 64, 128),
            vmem(6, 16, 128),
            vmem(2, 6, 16, 128),
            vmem(6, 4, 4, 16, 128),
            vmem(6, 16, 16, 128),
            vmem(6, 8, 2, 16, 128),
            vmem(3, 2, 256, 128),
            vmem(3, 2, 8, 32, 128),
            vmem(3, 6, 128, 128),
            vmem(3, 2, 8, 32, 128),
            vmem(3, 2, 256, 128),
            vmem(6, 8, 2, 16, 128),
            vmem(6, 16, 16, 128),
            vmem(6, 4, 64, 128),
            pltpu.SemaphoreType.DMA((7,)),
            pltpu.SemaphoreType.DMA((6, 6)),
            pltpu.SemaphoreType.DMA((6, 6)),
            pltpu.SemaphoreType.DMA((7,)),
        ],
        compiler_params=pltpu.CompilerParams(
            collective_id=0, has_side_effects=True, vmem_limit_bytes=62 * 1024 * 1024
        ),
    )(
        magnetization, kernel, jnp.asarray(tabz), jnp.asarray(taby), jnp.asarray(tabx),
        jnp.asarray(lam), jnp.asarray(lamx),
    )
    return pl.pallas_call(
        advance,
        out_shape=[jax.ShapeDtypeStruct(shape, F32)] * 2,
        in_specs=[in_vmem, in_vmem, pl.BlockSpec(memory_space=pltpu.SMEM)],
        out_specs=[anywhere] * 2,
        scratch_shapes=[vmem(*shape), vmem(*shape), pltpu.SemaphoreType.DMA((4, 2))],
        compiler_params=pltpu.CompilerParams(vmem_limit_bytes=16 * 1024 * 1024),
    )(m, demag, applied)


def solution(mesh):
    return jax.shard_map(
        shards,
        mesh=mesh,
        in_specs=(P(None, "gx", "gy", "gz"), P(None, ("gx", "gz"), "gy", None), P()),
        out_specs=(P(None, "gx", "gy", "gz"), P(None, "gx", "gy", "gz")),
        check_vma=False,
    )
```

```python
import math

import jax
import jax.numpy as jnp
import numpy as np
from jax import lax
from jax.experimental import pallas as pl
from jax.experimental.pallas import tpu as pltpu
from jax.sharding import PartitionSpec as P

MESH = pl.DeviceIdType.MESH
F32 = jnp.float32
BF16 = jnp.bfloat16
NX, NY, NZ = 64, 256, 512
EXCHANGE = 1.0
DAMPING = 0.3
STEP = 0.2
INVERSE_COUNT = 1.0 / (NX * NY * NZ)


def wave_z(block, slot):
    odd = slot >= 16
    return 64 * block + 2 * (slot % 16) + np.where(odd, 1, np.where(block >= 4, 2, 0))


def turn(rows, cols, length):
    angle = 2.0 * np.pi / length * ((rows[:, None] * cols[None, :]) % length)
    return np.cos(angle), np.sin(angle)


def grid(*counts):
    return [a.reshape(-1) for a in np.meshgrid(*(np.arange(n) for n in counts), indexing="ij")]


def z_tables():
    forward, backward = [], []
    for parity in range(2):
        block, part, slot = grid(8, 2, 16)
        cosine, sine = turn(np.arange(NZ // 2), wave_z(block, slot + 16 * parity), NZ)
        table = np.where(part == 0, cosine, -sine)
        weight = np.full(256, 2.0)
        if parity == 0:
            packed = (block == 0) & (slot == 0)
            alternate = 1.0 - 2.0 * (np.arange(NZ // 2) % 2)
            table[:, packed & (part == 1)] = alternate[:, None]
            weight[packed] = 1.0
        forward.append(table)
        backward.append(weight[:, None] * table.T)
    return forward, backward


def wave_y(owner, tile, group):
    return 128 * (tile // 2) + 16 * owner + 8 * (tile % 2) + group


def y_tables():
    forward, backward = [], []
    for parity in range(2):
        group, owner, tile = grid(4, 8, 4)
        half, block, row = grid(2, 4, 16)
        tables = turn(wave_y(owner, tile, 2 * group + parity), 32 * block + 16 * half + row, NY)
        forward.append(np.concatenate(tables, axis=0))
        backward.append(np.concatenate([t.T for t in tables], axis=0))
    return forward, backward


def x_tables():
    part, kx = grid(2, 64)
    parity, owner, xs, xp = grid(2, 8, 4, 2)
    cosine, sine = turn(kx, 4 * owner + xs, NX)
    out_re, in_re = (part == 0)[:, None], (xp == 0)[None, :]
    mine = kx[:, None] % 2 == parity[None, :]
    forward = np.where(mine, np.where(out_re == in_re, cosine, np.where(out_re, sine, -sine)), 0.0)
    mirrored = np.where(in_re, forward, -forward)
    backward = np.where(mine, np.where(out_re == in_re, cosine, np.where(in_re, -sine, sine)), 0.0).T
    return forward, mirrored, backward


def eigen_tables():
    lam = lambda k, n: 2.0 * np.cos(2.0 * np.pi * k / n) - 2.0
    owner, parity, block, tile, group, slot = grid(8, 2, 8, 4, 8, 16)
    ky, kz = wave_y(owner, tile, group), wave_z(block, slot + 16 * parity)
    z_part = lam(kz, NZ)
    packed = (block == 0) & (parity == 0) & (slot == 0)
    z_part = np.where(packed, np.where(ky % 128 == 0, -2.0, np.where(ky > 128, -4.0, 0.0)), z_part)
    table = (lam(ky, NY) + z_part) * EXCHANGE
    return (
        table.reshape(128, 4, 128).astype(np.float32),
        np.broadcast_to((lam(np.arange(64), NX) * EXCHANGE)[:, None], (64, 128)).astype(np.float32),
    )


def halves(table):
    table = np.asarray(table, np.float64)
    high = table.astype(np.float32).astype(jnp.bfloat16)
    low = (table - high.astype(np.float64)).astype(np.float32).astype(jnp.bfloat16)
    return np.stack([high, low])


def left_halves(table):
    high, low = halves(table)
    return np.concatenate([high, high, low], axis=1)


def split(value):
    high = value.astype(BF16)
    return high, (value - high.astype(F32)).astype(BF16)


def dot(a, b):
    return jnp.dot(a, b, preferred_element_type=F32)


def right_product(value, table, index):
    high, low = split(value)
    rows = value.shape[0]
    both = dot(jnp.concatenate([high, low], axis=0), table[index, 0])
    return both[:rows] + both[rows:] + dot(high, table[index, 1])


def left_product(table, index, value):
    high, low = split(value)
    return dot(table[index], jnp.concatenate([high, low, high], axis=0))


def wide_product(table, index, value):
    high, low = split(value)
    cols = value.shape[1]
    both = dot(table[index, 0], jnp.concatenate([high, low], axis=1))
    return both[:, :cols] + both[:, cols:] + dot(table[index, 1], high)


def swap_lanes(values):
    values = list(values)
    lane = lax.broadcasted_iota(jnp.int32, values[0].shape, 1)
    step = len(values) // 2
    width = 64
    while step:
        low = (lane & width) == 0
        for i in range(len(values)):
            if i & step == 0:
                a, b = values[i], values[i + step]
                values[i] = jnp.where(low, a, pltpu.roll(b, width, 1))
                values[i + step] = jnp.where(low, pltpu.roll(a, 128 - width, 1), b)
        step //= 2
        width //= 2
    return values


PAIR = ((0, 3, 4), (3, 1, 5), (4, 5, 2))
FORWARD, BACKWARD = 0, 2
XF, XM, XB = range(3)


def transform(
    m_hbm, k_hbm, tabz_hbm, taby_hbm, tabx_hbm, lam_hbm, lamx_hbm,
    m, r6,
    kraw, tabz, tabyf, tabyb, tabx, lam, lamx, kp, k2, kq, kn_out, kn_in,
    r1, s2, r2, s3, r3, spec, s4, r4, s5, r5, s6,
    local_sem, send_sem, recv_sem, kn_sems,
):
    gx, gy, gz = lax.axis_index("gx"), lax.axis_index("gy"), lax.axis_index("gz")
    core, top = lax.rem(gx, 2), gx // 2
    place_xy = 2 * gy + top
    place_z = 4 * core + gz
    load_m = pltpu.make_async_copy(m_hbm, m, local_sem.at[0])
    load_m.start()
    load_k = pltpu.make_async_copy(k_hbm, kraw, local_sem.at[1])
    load_k.start()

    by_y = lambda p: {"gy": p}
    on_z = [(z, {"gz": z}) for z in (lax.rem(gz + d, 4) for d in (2, 1, 3))]
    on_xy = [
        (2 * y + x, {"gx": 2 * x + core, "gy": y})
        for y, x in (
            (4 * lax.rem(gy // 4 + p, 2) + lax.rem(gy + d, 4), lax.rem(top + f, 2))
            for p, d, f in (
                (1, 2, 0), (1, 1, 0), (1, 3, 0), (1, 2, 1), (0, 2, 1), (1, 0, 0), (1, 1, 1), (1, 3, 1),
                (0, 1, 1), (0, 3, 1), (0, 2, 0), (1, 0, 1), (0, 0, 1), (0, 1, 0), (0, 3, 0),
            )
        )
    ]
    on_cz = [
        (4 * k + z, {"gx": 2 * top + k, "gz": z})
        for k, z in (
            (lax.rem(core + k, 2), lax.rem(gz + d, 4)) for d in (2, 1, 3, 0) for k in (1, 0) if (d, k) != (0, 0)
        )
    ]

    barrier = pltpu.get_barrier_semaphore()

    def repeat(start, stop, step):
        def one(j, carry):
            step(j)
            return carry

        lax.fori_loop(start, stop, one, 0)

    for _, device in on_xy + on_cz:
        pl.semaphore_signal(barrier, inc=1, device_id=device, device_id_type=MESH)
    pl.semaphore_wait(barrier, 22)

    def copy(e, n, src, dst, device):
        return pltpu.make_async_remote_copy(
            src_ref=src, dst_ref=dst, send_sem=send_sem.at[e, n], recv_sem=recv_sem.at[e, n],
            device_id=device, device_id_type=MESH,
        )

    def send_all(e, n, src, dst, me, others):
        for p, device in others:
            copy(e, n, src.at[n, p], dst.at[n, me], device).start()
        dst[n, me] = src[n, me]

    def arrived(e, n, dst, count):
        part = dst.at[n, pl.ds(0, count - 1)]
        copy(e, n, part, part, by_y(lax.rem(gy + 1, 8))).wait_recv()

    def send_both(e, c, src, dst):
        for p, device in on_cz:
            copy(e, c, src.at[c, :, p], dst.at[c, :, place_z], device).start()
        dst[c, :, place_z] = src[c, :, place_z]

    def both_arrived(e, c, dst):
        part = dst.at[c, :, pl.ds(0, 7)]
        copy(e, c, part, part, by_y(lax.rem(gy + 1, 8))).wait_recv()

    load_m.wait()
    m_blocks = m.reshape(3, 4, 4, 32, 128)

    def send_m(n):
        c, half = n // 2, lax.rem(n, 2)
        rows = pl.ds(pl.multiple_of(16 * half, 16), 16)

        for p, device in on_z:
            copy(0, n, m_blocks.at[c, p, :, rows, :], r1.at[n, gz], device).start()
        r1[n, gz] = m_blocks[c, gz, :, rows, :]

    repeat(0, 6, send_m)

    loads = [
        pltpu.make_async_copy(tabz_hbm, tabz, local_sem.at[0]),
        pltpu.make_async_copy(lam_hbm.at[(2 * place_z + top) * 8 + gy], lam, local_sem.at[2]),
        pltpu.make_async_copy(lamx_hbm, lamx, local_sem.at[3]),
        pltpu.make_async_copy(taby_hbm.at[0:2], tabyf, local_sem.at[4]),
        pltpu.make_async_copy(tabx_hbm, tabx, local_sem.at[5]),
        pltpu.make_async_copy(taby_hbm.at[2:4], tabyb, local_sem.at[6]),
    ]
    for load in loads:
        load.start()

    load_k.wait()
    late = gy >= 4
    first = gy == 0

    def prepare(cc):
        for v in range(2):
            own, other = [], []
            for g in range(8):
                i = 8 * v + g
                even = kraw[cc, i, pl.ds(0, 16, stride=2), :]
                even = jnp.where(late, kraw[cc, i, pl.ds(2, 16, stride=2), :], even)
                odd = kraw[cc, i, pl.ds(1, 16, stride=2), :]
                own.append(jnp.where(top == 1, odd, even))
                other.append(jnp.where(top == 1, even, odd))
            kp[cc, 2 * top + v] = -INVERSE_COUNT * jnp.concatenate(own, axis=0).T
            kq[cc, v] = -INVERSE_COUNT * jnp.concatenate(other, axis=0).T

    def share(n, start, count):
        part = pl.ds(start, count)
        return pltpu.make_async_remote_copy(
            src_ref=kq.at[part], dst_ref=kp.at[part, pl.ds(2 * top, 2)],
            send_sem=kn_sems.at[n], recv_sem=kn_sems.at[n + 1],
            device_id={"gx": lax.rem(gx + 2, 4)}, device_id_type=MESH,
        )

    shares = [share(0, 0, 2), share(2, 2, 4)]
    repeat(0, 2, prepare)
    shares[0].start()

    def nyquist(n):
        return pltpu.make_async_remote_copy(
            src_ref=kn_out, dst_ref=kn_in.at[n], send_sem=kn_sems.at[4], recv_sem=kn_sems.at[5 + n],
            device_id={"gx": core, "gy": 0}, device_id_type=MESH,
        )

    @pl.when(gy == 4)
    def _():
        for cc in range(6):
            for i in range(16):
                kn_out[cc, i : i + 1, 0:64] = kraw[cc, i, 0:1, :]
        nyquist(top).start()

    repeat(2, 6, prepare)
    loads[0].wait()

    def z_forward(n):
        arrived(0, n, r1, 4)
        near = [r1[n, s].reshape(64, 128) for s in range(2)]
        far = [r1[n, s + 2].reshape(64, 128) for s in range(2)]
        out = [
            right_product(jnp.concatenate([a + b for a, b in zip(near, far)], axis=1), tabz, FORWARD),
            right_product(jnp.concatenate([a - b for a, b in zip(near, far)], axis=1), tabz, FORWARD + 1),
        ]
        for parity in range(2):
            for t in range(2):
                parts = swap_lanes(
                    [out[parity][16 * x : 16 * x + 16, 128 * t : 128 * t + 128] for x in range(4)]
                )
                for q in range(4):
                    s2[n, 2 * (4 * t + q) + parity] = parts[q]
        send_all(1, n, s2, r2_blocks, place_xy, on_xy)

    r2_blocks = r2.reshape(6, 16, 16, 128)
    s5_blocks = s5.reshape(6, 16, 16, 128)
    repeat(0, 6, z_forward)
    shares[1].start()

    for load in loads[1:]:
        load.wait()
    row = lax.broadcasted_iota(jnp.int32, (128, 128), 0)
    lane = lax.broadcasted_iota(jnp.int32, (128, 128), 1)
    real = (lane & 16) == 0
    packed_lane = first & (top == 0) & ((lane & 15) == 0)
    low = (row & 2) == 0
    lone = ((row & 125) == 0, row < 0)
    from_imag = lambda z: pltpu.roll(z, 112, 1)
    from_real = lambda z: pltpu.roll(z, 16, 1)
    partner = lambda z: jnp.where(real, from_imag(z), from_real(z))

    def y_forward(c):
        arrived(1, 2 * c, r2_blocks, 16)
        arrived(1, 2 * c + 1, r2_blocks, 16)
        part = lambda h, x: r2[pl.ds(2 * c, 2), 4 * h : 4 * h + 4, x].reshape(128, 128)
        halves_x = []
        for h in range(2):
            a, b = part(h, 0), part(h, 1)
            halves_x.append(jnp.concatenate([a + b, a - b], axis=1))
        out = [[], []]
        for parity, value in enumerate((halves_x[0] + halves_x[1], halves_x[0] - halves_x[1])):
            rows = wide_product(tabyf, parity, value)
            for e in range(2):
                cosine, sine = rows[:128, 128 * e : 128 * e + 128], rows[128:, 128 * e : 128 * e + 128]
                turned = partner(sine)
                plain = cosine + jnp.where(real, turned, -turned)
                single = jnp.where(
                    low, jnp.where(real, cosine, -turned), jnp.where(real, from_imag(cosine), -sine)
                )
                out[e].append(jnp.where(packed_lane & ~lone[parity], single, plain))
        for e in range(2):
            parts = swap_lanes([out[e][g % 2][32 * (g // 2) : 32 * (g // 2) + 32] for g in range(8)])
            for x in range(8):
                s3[c, e, pl.ds(x, 32, stride=8), :] = parts[x]
        send_both(2, c, s3_blocks, r3)

    s3_blocks = s3.reshape(3, 2, 8, 32, 128)
    r4_blocks = r4.reshape(3, 2, 8, 32, 128)
    repeat(0, 3, y_forward)

    def x_forward(c):
        both_arrived(2, c, r3)
        tiles = [r3[c, :, :, 8 * v : 8 * v + 8, :].reshape(128, 128) for v in range(4)]
        out = left_product(tabx, XF, jnp.concatenate(tiles, axis=1))
        for v in range(4):
            spec[c, v] = out[:, 128 * v : 128 * v + 128]
        out = left_product(tabx, XM, jnp.concatenate(tiles[::2], axis=1))
        for j in range(2):
            spec[c, 4 + j] = out[:, 128 * j : 128 * j + 128]

    repeat(0, 2, x_forward)

    for piece in shares:
        piece.wait_recv()
    k2[...] = jnp.zeros_like(k2)

    @pl.when(first & (top == 0))
    def _():
        for n in range(2):
            nyquist(n).wait_recv()
        small_lane = lax.broadcasted_iota(jnp.int32, (64, 128), 1)
        corner_lane = (place_z == 0) & (small_lane == 0)

        def mend(cc):
            for v in range(4):
                rows = [
                    jnp.broadcast_to(kn_in[v // 2, cc, i : i + 1, 0:64], (16, 64))
                    for i in range(8 * (v % 2), 8 * (v % 2) + 8)
                ]
                edge = -INVERSE_COUNT * jnp.concatenate(rows, axis=0).T
                plain = kp[cc, v]
                value = jnp.where((small_lane & 15) == 0, edge, plain) if v >= 2 else plain
                if v % 2 == 0:
                    value = jnp.where(corner_lane, 0.5 * (plain + edge), value)
                    term = jnp.where(cc < 3, 2.0 * EXCHANGE * INVERSE_COUNT, 0.0)
                    k2[cc, v // 2] = jnp.where(corner_lane, 0.5 * (plain - edge) + term, 0.0)
                kp[cc, v] = value

        repeat(0, 6, mend)

    for cc in range(3):
        for v in range(4):
            kp[cc, v] += INVERSE_COUNT * (lamx[...] + lam[v : v + 1, :])
    x_forward(2)

    for c in range(3):
        tiles = []
        for v in range(4):
            terms = []
            for part in range(2):
                rows = slice(64 * part, 64 * part + 64)
                total = sum(kp[PAIR[c][d], v] * spec[d, v, rows, :] for d in range(3))
                if v % 2 == 0:
                    total = total + sum(
                        k2[PAIR[c][d], v // 2] * spec[d, 4 + v // 2, rows, :] for d in range(3)
                    )
                terms.append(total)
            tiles.append(jnp.concatenate(terms, axis=0))
        out = left_product(tabx, XB, jnp.concatenate(tiles, axis=1))
        for v in range(4):
            s4[c, :, :, 8 * v : 8 * v + 8, :] = out[:, 128 * v : 128 * v + 128].reshape(2, 8, 8, 128)
        send_both(3, c, s4, r4_blocks)

    alternate = (1 - 2 * (row & 1)).astype(F32)

    def y_backward(c):
        both_arrived(3, c, r4_blocks)
        pieces = [swap_lanes([r4[c, e, pl.ds(x, 32, stride=8), :] for x in range(8)]) for e in range(2)]
        out = [[], []]
        for parity in range(2):
            value = [
                jnp.concatenate([pieces[e][2 * g + parity] for g in range(4)], axis=0) for e in range(2)
            ]
            masked = jnp.concatenate([jnp.where(low & ~lone[parity], z, 0.0) for z in value], axis=1)
            rows = wide_product(tabyb, parity, jnp.concatenate(value, axis=1))
            rows_low = wide_product(tabyb, parity, masked)
            for e in range(2):
                cols = slice(128 * e, 128 * e + 128)
                cosine, sine = rows[:128, cols], rows[128:, cols]
                cosine_low, sine_low = rows_low[:128, cols], rows_low[128:, cols]
                turned = partner(sine)
                plain = cosine + jnp.where(real, -turned, turned)
                cosine_high, sine_high = cosine - cosine_low, sine - sine_low
                base = 0.0
                if parity == 0:
                    base = value[e][0:1, :] + alternate * value[e][2:3, :]
                    cosine_high = cosine_high - base
                double = jnp.where(real, cosine_low - from_imag(sine_low), from_real(cosine_high) - sine_high)
                out[e].append(jnp.where(packed_lane, 2.0 * double + base, plain))
        for h in range(2):
            even, odd = [out[e][0] + out[e][1] if h == 0 else out[e][0] - out[e][1] for e in range(2)]
            for x, value in enumerate((even + odd, even - odd)):
                s5[pl.ds(2 * c, 2), 4 * h : 4 * h + 4, x] = value.reshape(2, 4, 16, 128)
        send_all(4, 2 * c, s5_blocks, r5, place_xy, on_xy)
        send_all(4, 2 * c + 1, s5_blocks, r5, place_xy, on_xy)

    repeat(0, 3, y_backward)

    def z_backward(n):
        arrived(4, n, r5, 16)
        tiles = [[], []]
        for parity in range(2):
            for t in range(2):
                parts = swap_lanes([r5[n, 2 * (4 * t + q) + parity] for q in range(4)])
                tiles[parity].append(jnp.concatenate(parts, axis=0))
        out = [right_product(jnp.concatenate(tiles[p], axis=1), tabz, BACKWARD + p) for p in range(2)]
        for h, value in enumerate((out[0] + out[1], out[0] - out[1])):
            s6[n, 2 * h] = value[:, 0:128]
            s6[n, 2 * h + 1] = value[:, 128:256]
        send_all(5, n, s6, r6, gz, on_z)

    repeat(0, 6, z_backward)

    def sent(e, chunks, part):
        repeat(0, chunks, lambda n: copy(e, n, part(n), part(n), by_y(lax.rem(gy + 1, 8))).wait_send())

    sent(0, 6, lambda n: r1.at[n, pl.ds(0, 3)])
    sent(1, 6, lambda n: s2.at[n, pl.ds(0, 15)])
    sent(2, 3, lambda n: s3_blocks.at[n, :, pl.ds(0, 7)])
    sent(3, 3, lambda n: s4.at[n, :, pl.ds(0, 7)])
    sent(4, 6, lambda n: s5_blocks.at[n, pl.ds(0, 15)])
    for piece in shares:
        piece.wait_send()

    @pl.when(gy == 4)
    def _():
        nyquist(top).wait_send()

    repeat(0, 6, lambda n: arrived(5, n, r6, 4))
    sent(5, 6, lambda n: s6.at[n, pl.ds(0, 3)])


def advance(m, demag, applied, pred_hbm, torque_hbm, pout, tout, sems):
    cross = lambda a, b: [
        a[1] * b[2] - a[2] * b[1],
        a[2] * b[0] - a[0] * b[2],
        a[0] * b[1] - a[1] * b[0],
    ]
    stores = []
    for s in range(4):
        planes = slice(4 * s, 4 * s + 4)
        for half in range(2):
            rows = slice(16 * half, 16 * half + 16)
            mag = [m[c, planes, rows, :] for c in range(3)]
            field = [demag[2 * c + half, s].reshape(4, 16, 128) + applied[c] for c in range(3)]
            precess = cross(mag, field)
            twist = cross(mag, precess)
            torque = [-(precess[c] + DAMPING * twist[c]) / (1.0 + DAMPING * DAMPING) for c in range(3)]
            stepped = [mag[c] + STEP * torque[c] for c in range(3)]
            length = jnp.sqrt(stepped[0] * stepped[0] + stepped[1] * stepped[1] + stepped[2] * stepped[2])
            for c in range(3):
                tout[c, planes, rows, :] = torque[c]
                pout[c, planes, rows, :] = stepped[c] / length
        stores += [
            pltpu.make_async_copy(tout.at[:, planes], torque_hbm.at[:, planes], sems.at[s, 0]),
            pltpu.make_async_copy(pout.at[:, planes], pred_hbm.at[:, planes], sems.at[s, 1]),
        ]
        stores[-2].start()
        stores[-1].start()
    for store in stores:
        store.wait()


def shards(magnetization, kernel, applied):
    zf, zb = z_tables()
    yf, yb = y_tables()
    tabz = np.stack([halves(t) for t in zf + zb])
    taby = np.stack([halves(t) for t in yf + yb])
    tabx = np.stack([left_halves(t) for t in x_tables()])
    lam, lamx = eigen_tables()
    shape = magnetization.shape
    anywhere = pl.BlockSpec(memory_space=pltpu.HBM)
    in_vmem = pl.BlockSpec(memory_space=pltpu.VMEM)
    vmem = lambda *shape, dtype=F32: pltpu.VMEM(shape, dtype)
    m, demag = pl.pallas_call(
        transform,
        out_shape=[vmem(*shape), vmem(6, 4, 64, 128)],
        in_specs=[anywhere] * 7,
        out_specs=[in_vmem, in_vmem],
        scratch_shapes=[
            vmem(6, 16, 64, 64),
            vmem(4, 2, 256, 256, dtype=BF16),
            vmem(2, 2, 256, 128, dtype=BF16),
            vmem(2, 2, 256, 128, dtype=BF16),
            vmem(3, 128, 384, dtype=BF16),
            vmem(4, 128),
            vmem(64, 128),
            vmem(6, 4, 64, 128),
            vmem(6, 2, 64, 128),
            vmem(6, 2, 64, 128),
            vmem(6, 16, 128),
            vmem(2, 6, 16, 128),
            vmem(6, 4, 4, 16, 128),
            vmem(6, 16, 16, 128),
            vmem(6, 8, 2, 16, 128),
            vmem(3, 2, 256, 128),
            vmem(3, 2, 8, 32, 128),
            vmem(3, 6, 128, 128),
            vmem(3, 2, 8, 32, 128),
            vmem(3, 2, 256, 128),
            vmem(6, 8, 2, 16, 128),
            vmem(6, 16, 16, 128),
            vmem(6, 4, 64, 128),
            pltpu.SemaphoreType.DMA((7,)),
            pltpu.SemaphoreType.DMA((6, 6)),
            pltpu.SemaphoreType.DMA((6, 6)),
            pltpu.SemaphoreType.DMA((7,)),
        ],
        compiler_params=pltpu.CompilerParams(
            collective_id=0, has_side_effects=True, vmem_limit_bytes=62 * 1024 * 1024
        ),
    )(
        magnetization, kernel, jnp.asarray(tabz), jnp.asarray(taby), jnp.asarray(tabx),
        jnp.asarray(lam), jnp.asarray(lamx),
    )
    return pl.pallas_call(
        advance,
        out_shape=[jax.ShapeDtypeStruct(shape, F32)] * 2,
        in_specs=[in_vmem, in_vmem, pl.BlockSpec(memory_space=pltpu.SMEM)],
        out_specs=[anywhere] * 2,
        scratch_shapes=[vmem(*shape), vmem(*shape), pltpu.SemaphoreType.DMA((4, 2))],
        compiler_params=pltpu.CompilerParams(vmem_limit_bytes=16 * 1024 * 1024),
    )(m, demag, applied)


def solution(mesh):
    return jax.shard_map(
        shards,
        mesh=mesh,
        in_specs=(P(None, "gx", "gy", "gz"), P(None, ("gx", "gz"), "gy", None), P()),
        out_specs=(P(None, "gx", "gy", "gz"), P(None, "gx", "gy", "gz")),
        check_vma=False,
    )
```

```python
import math

import jax
import jax.numpy as jnp
import numpy as np
from jax import lax
from jax.experimental import pallas as pl
from jax.experimental.pallas import tpu as pltpu
from jax.sharding import PartitionSpec as P

MESH = pl.DeviceIdType.MESH
F32 = jnp.float32
BF16 = jnp.bfloat16
NX, NY, NZ = 64, 256, 512
EXCHANGE = 1.0
DAMPING = 0.3
STEP = 0.2
INVERSE_COUNT = 1.0 / (NX * NY * NZ)


def wave_z(block, slot):
    odd = slot >= 16
    return 64 * block + 2 * (slot % 16) + np.where(odd, 1, np.where(block >= 4, 2, 0))


def turn(rows, cols, length):
    angle = 2.0 * np.pi / length * ((rows[:, None] * cols[None, :]) % length)
    return np.cos(angle), np.sin(angle)


def grid(*counts):
    return [a.reshape(-1) for a in np.meshgrid(*(np.arange(n) for n in counts), indexing="ij")]


def z_tables():
    forward, backward = [], []
    for parity in range(2):
        block, part, slot = grid(8, 2, 16)
        cosine, sine = turn(np.arange(NZ // 2), wave_z(block, slot + 16 * parity), NZ)
        table = np.where(part == 0, cosine, -sine)
        weight = np.full(256, 2.0)
        if parity == 0:
            packed = (block == 0) & (slot == 0)
            alternate = 1.0 - 2.0 * (np.arange(NZ // 2) % 2)
            table[:, packed & (part == 1)] = alternate[:, None]
            weight[packed] = 1.0
        forward.append(table)
        backward.append(weight[:, None] * table.T)
    return forward, backward


def wave_y(owner, tile, group):
    return 128 * (tile // 2) + 16 * owner + 8 * (tile % 2) + group


def y_tables():
    forward, backward = [], []
    for parity in range(2):
        group, owner, tile = grid(4, 8, 4)
        half, block, row = grid(2, 4, 16)
        tables = turn(wave_y(owner, tile, 2 * group + parity), 32 * block + 16 * half + row, NY)
        forward.append(np.concatenate(tables, axis=0))
        backward.append(np.concatenate([t.T for t in tables], axis=0))
    return forward, backward


def x_tables():
    part, kx = grid(2, 64)
    parity, owner, xs, xp = grid(2, 8, 4, 2)
    cosine, sine = turn(kx, 4 * owner + xs, NX)
    out_re, in_re = (part == 0)[:, None], (xp == 0)[None, :]
    mine = kx[:, None] % 2 == parity[None, :]
    forward = np.where(mine, np.where(out_re == in_re, cosine, np.where(out_re, sine, -sine)), 0.0)
    mirrored = np.where(in_re, forward, -forward)
    backward = np.where(mine, np.where(out_re == in_re, cosine, np.where(in_re, -sine, sine)), 0.0).T
    return forward, mirrored, backward


def eigen_tables():
    lam = lambda k, n: 2.0 * np.cos(2.0 * np.pi * k / n) - 2.0
    owner, parity, block, tile, group, slot = grid(8, 2, 8, 4, 8, 16)
    ky, kz = wave_y(owner, tile, group), wave_z(block, slot + 16 * parity)
    z_part = lam(kz, NZ)
    packed = (block == 0) & (parity == 0) & (slot == 0)
    z_part = np.where(packed, np.where(ky % 128 == 0, -2.0, np.where(ky > 128, -4.0, 0.0)), z_part)
    table = (lam(ky, NY) + z_part) * EXCHANGE
    return (
        table.reshape(128, 4, 128).astype(np.float32),
        np.broadcast_to((lam(np.arange(64), NX) * EXCHANGE)[:, None], (64, 128)).astype(np.float32),
    )


def halves(table):
    table = np.asarray(table, np.float64)
    high = table.astype(np.float32).astype(jnp.bfloat16)
    low = (table - high.astype(np.float64)).astype(np.float32).astype(jnp.bfloat16)
    return np.stack([high, low])


def left_halves(table):
    high, low = halves(table)
    return np.concatenate([high, high, low], axis=1)


def split(value):
    high = value.astype(BF16)
    return high, (value - high.astype(F32)).astype(BF16)


def dot(a, b):
    return jnp.dot(a, b, preferred_element_type=F32)


def right_product(value, table, index):
    high, low = split(value)
    rows = value.shape[0]
    both = dot(jnp.concatenate([high, low], axis=0), table[index, 0])
    return both[:rows] + both[rows:] + dot(high, table[index, 1])


def left_product(table, index, value):
    high, low = split(value)
    return dot(table[index], jnp.concatenate([high, low, high], axis=0))


def wide_product(table, index, value):
    high, low = split(value)
    cols = value.shape[1]
    both = dot(table[index, 0], jnp.concatenate([high, low], axis=1))
    return both[:, :cols] + both[:, cols:] + dot(table[index, 1], high)


def swap_lanes(values):
    values = list(values)
    lane = lax.broadcasted_iota(jnp.int32, values[0].shape, 1)
    step = len(values) // 2
    width = 64
    while step:
        low = (lane & width) == 0
        for i in range(len(values)):
            if i & step == 0:
                a, b = values[i], values[i + step]
                values[i] = jnp.where(low, a, pltpu.roll(b, width, 1))
                values[i + step] = jnp.where(low, pltpu.roll(a, 128 - width, 1), b)
        step //= 2
        width //= 2
    return values


PAIR = ((0, 3, 4), (3, 1, 5), (4, 5, 2))
FORWARD, BACKWARD = 0, 2
XF, XM, XB = range(3)


def transform(
    m_hbm, k_hbm, tabz_hbm, taby_hbm, tabx_hbm, lam_hbm, lamx_hbm,
    m, r6,
    kraw, tabz, tabyf, tabyb, tabx, lam, lamx, kp, k2, kq, kn_out, kn_in,
    r1, s2, r2, s3, r3, spec, s4, r4, s5, r5, s6,
    local_sem, send_sem, recv_sem, kn_sems,
):
    gx, gy, gz = lax.axis_index("gx"), lax.axis_index("gy"), lax.axis_index("gz")
    core, top = lax.rem(gx, 2), gx // 2
    place_xy = 2 * gy + top
    place_z = 4 * core + gz
    load_m = pltpu.make_async_copy(m_hbm, m, local_sem.at[0])
    load_m.start()
    load_k = pltpu.make_async_copy(k_hbm, kraw, local_sem.at[1])
    load_k.start()

    by_y = lambda p: {"gy": p}
    on_z = [(z, {"gz": z}) for z in (lax.rem(gz + d, 4) for d in (2, 1, 3))]
    on_xy = [
        (2 * y + x, {"gx": 2 * x + core, "gy": y})
        for y, x in (
            (4 * lax.rem(gy // 4 + p, 2) + lax.rem(gy + d, 4), lax.rem(top + f, 2))
            for p, d, f in (
                (1, 2, 0), (1, 1, 0), (1, 3, 0), (1, 2, 1), (0, 2, 1), (1, 0, 0), (1, 1, 1), (1, 3, 1),
                (0, 1, 1), (0, 3, 1), (0, 2, 0), (1, 0, 1), (0, 0, 1), (0, 1, 0), (0, 3, 0),
            )
        )
    ]
    on_cz = [
        (4 * k + z, {"gx": 2 * top + k, "gz": z})
        for k, z in (
            (lax.rem(core + k, 2), lax.rem(gz + d, 4)) for d in (2, 1, 3, 0) for k in (1, 0) if (d, k) != (0, 0)
        )
    ]

    barrier = pltpu.get_barrier_semaphore()

    def repeat(start, stop, step):
        def one(j, carry):
            step(j)
            return carry

        lax.fori_loop(start, stop, one, 0)

    for _, device in on_xy + on_cz:
        pl.semaphore_signal(barrier, inc=1, device_id=device, device_id_type=MESH)
    pl.semaphore_wait(barrier, 22)

    def copy(e, n, src, dst, device):
        return pltpu.make_async_remote_copy(
            src_ref=src, dst_ref=dst, send_sem=send_sem.at[e, n], recv_sem=recv_sem.at[e, n],
            device_id=device, device_id_type=MESH,
        )

    def send_all(e, n, src, dst, me, others):
        for p, device in others:
            copy(e, n, src.at[n, p], dst.at[n, me], device).start()
        dst[n, me] = src[n, me]

    def arrived(e, n, dst, count):
        part = dst.at[n, pl.ds(0, count - 1)]
        copy(e, n, part, part, by_y(lax.rem(gy + 1, 8))).wait_recv()

    def send_both(e, c, src, dst):
        for p, device in on_cz:
            copy(e, c, src.at[c, :, p], dst.at[c, :, place_z], device).start()
        dst[c, :, place_z] = src[c, :, place_z]

    def both_arrived(e, c, dst):
        part = dst.at[c, :, pl.ds(0, 7)]
        copy(e, c, part, part, by_y(lax.rem(gy + 1, 8))).wait_recv()

    load_m.wait()
    m_blocks = m.reshape(3, 4, 4, 32, 128)

    def send_m(n):
        c, half = n // 2, lax.rem(n, 2)
        rows = pl.ds(pl.multiple_of(16 * half, 16), 16)

        for p, device in on_z:
            copy(0, n, m_blocks.at[c, p, :, rows, :], r1.at[n, gz], device).start()
        r1[n, gz] = m_blocks[c, gz, :, rows, :]

    repeat(0, 6, send_m)

    loads = [
        pltpu.make_async_copy(tabz_hbm, tabz, local_sem.at[0]),
        pltpu.make_async_copy(lam_hbm.at[(2 * place_z + top) * 8 + gy], lam, local_sem.at[2]),
        pltpu.make_async_copy(lamx_hbm, lamx, local_sem.at[3]),
        pltpu.make_async_copy(taby_hbm.at[0:2], tabyf, local_sem.at[4]),
        pltpu.make_async_copy(tabx_hbm, tabx, local_sem.at[5]),
        pltpu.make_async_copy(taby_hbm.at[2:4], tabyb, local_sem.at[6]),
    ]
    for load in loads:
        load.start()

    load_k.wait()
    late = gy >= 4
    first = gy == 0

    def prepare(cc):
        for v in range(2):
            own, other = [], []
            for g in range(8):
                i = 8 * v + g
                even = kraw[cc, i, pl.ds(0, 16, stride=2), :]
                even = jnp.where(late, kraw[cc, i, pl.ds(2, 16, stride=2), :], even)
                odd = kraw[cc, i, pl.ds(1, 16, stride=2), :]
                own.append(jnp.where(top == 1, odd, even))
                other.append(jnp.where(top == 1, even, odd))
            kp[cc, 2 * top + v] = -INVERSE_COUNT * jnp.concatenate(own, axis=0).T
            kq[cc, v] = -INVERSE_COUNT * jnp.concatenate(other, axis=0).T

    def share(n, start, count):
        part = pl.ds(start, count)
        return pltpu.make_async_remote_copy(
            src_ref=kq.at[part], dst_ref=kp.at[part, pl.ds(2 * top, 2)],
            send_sem=kn_sems.at[n], recv_sem=kn_sems.at[n + 1],
            device_id={"gx": lax.rem(gx + 2, 4)}, device_id_type=MESH,
        )

    shares = [share(0, 0, 2), share(2, 2, 4)]
    repeat(0, 2, prepare)
    shares[0].start()

    def nyquist(n):
        return pltpu.make_async_remote_copy(
            src_ref=kn_out, dst_ref=kn_in.at[n], send_sem=kn_sems.at[4], recv_sem=kn_sems.at[5 + n],
            device_id={"gx": core, "gy": 0}, device_id_type=MESH,
        )

    @pl.when(gy == 4)
    def _():
        for cc in range(6):
            for i in range(16):
                kn_out[cc, i : i + 1, 0:64] = kraw[cc, i, 0:1, :]
        nyquist(top).start()

    repeat(2, 6, prepare)
    loads[0].wait()

    def z_forward(n):
        arrived(0, n, r1, 4)
        near = [r1[n, s].reshape(64, 128) for s in range(2)]
        far = [r1[n, s + 2].reshape(64, 128) for s in range(2)]
        out = [
            right_product(jnp.concatenate([a + b for a, b in zip(near, far)], axis=1), tabz, FORWARD),
            right_product(jnp.concatenate([a - b for a, b in zip(near, far)], axis=1), tabz, FORWARD + 1),
        ]
        for parity in range(2):
            for t in range(2):
                parts = swap_lanes(
                    [out[parity][16 * x : 16 * x + 16, 128 * t : 128 * t + 128] for x in range(4)]
                )
                for q in range(4):
                    s2[n, 2 * (4 * t + q) + parity] = parts[q]
        send_all(1, n, s2, r2_blocks, place_xy, on_xy)

    r2_blocks = r2.reshape(6, 16, 16, 128)
    s5_blocks = s5.reshape(6, 16, 16, 128)
    repeat(0, 6, z_forward)
    shares[1].start()

    for load in loads[1:]:
        load.wait()
    row = lax.broadcasted_iota(jnp.int32, (128, 128), 0)
    lane = lax.broadcasted_iota(jnp.int32, (128, 128), 1)
    real = (lane & 16) == 0
    packed_lane = first & (top == 0) & ((lane & 15) == 0)
    low = (row & 2) == 0
    lone = ((row & 125) == 0, row < 0)
    from_imag = lambda z: pltpu.roll(z, 112, 1)
    from_real = lambda z: pltpu.roll(z, 16, 1)
    partner = lambda z: jnp.where(real, from_imag(z), from_real(z))

    def y_forward(c):
        arrived(1, 2 * c, r2_blocks, 16)
        arrived(1, 2 * c + 1, r2_blocks, 16)
        part = lambda h, x: r2[pl.ds(2 * c, 2), 4 * h : 4 * h + 4, x].reshape(128, 128)
        halves_x = []
        for h in range(2):
            a, b = part(h, 0), part(h, 1)
            halves_x.append(jnp.concatenate([a + b, a - b], axis=1))
        out = [[], []]
        for parity, value in enumerate((halves_x[0] + halves_x[1], halves_x[0] - halves_x[1])):
            rows = wide_product(tabyf, parity, value)
            for e in range(2):
                cosine, sine = rows[:128, 128 * e : 128 * e + 128], rows[128:, 128 * e : 128 * e + 128]
                turned = partner(sine)
                plain = cosine + jnp.where(real, turned, -turned)
                single = jnp.where(
                    low, jnp.where(real, cosine, -turned), jnp.where(real, from_imag(cosine), -sine)
                )
                out[e].append(jnp.where(packed_lane & ~lone[parity], single, plain))
        for e in range(2):
            parts = swap_lanes([out[e][g % 2][32 * (g // 2) : 32 * (g // 2) + 32] for g in range(8)])
            for x in range(8):
                s3[c, e, pl.ds(x, 32, stride=8), :] = parts[x]
            for p, device in on_cz:
                copy(2, c, s3_blocks.at[c, e, p], r3.at[c, e, place_z], device).start()
        r3[c, :, place_z] = s3_blocks[c, :, place_z]

    s3_blocks = s3.reshape(3, 2, 8, 32, 128)
    r4_blocks = r4.reshape(3, 2, 8, 32, 128)
    repeat(0, 3, y_forward)

    def x_forward(c):
        both_arrived(2, c, r3)
        tiles = [r3[c, :, :, 8 * v : 8 * v + 8, :].reshape(128, 128) for v in range(4)]
        out = left_product(tabx, XF, jnp.concatenate(tiles, axis=1))
        for v in range(4):
            spec[c, v] = out[:, 128 * v : 128 * v + 128]
        out = left_product(tabx, XM, jnp.concatenate(tiles[::2], axis=1))
        for j in range(2):
            spec[c, 4 + j] = out[:, 128 * j : 128 * j + 128]

    repeat(0, 2, x_forward)

    for piece in shares:
        piece.wait_recv()
    k2[...] = jnp.zeros_like(k2)

    @pl.when(first & (top == 0))
    def _():
        for n in range(2):
            nyquist(n).wait_recv()
        small_lane = lax.broadcasted_iota(jnp.int32, (64, 128), 1)
        corner_lane = (place_z == 0) & (small_lane == 0)

        def mend(cc):
            for v in range(4):
                rows = [
                    jnp.broadcast_to(kn_in[v // 2, cc, i : i + 1, 0:64], (16, 64))
                    for i in range(8 * (v % 2), 8 * (v % 2) + 8)
                ]
                edge = -INVERSE_COUNT * jnp.concatenate(rows, axis=0).T
                plain = kp[cc, v]
                value = jnp.where((small_lane & 15) == 0, edge, plain) if v >= 2 else plain
                if v % 2 == 0:
                    value = jnp.where(corner_lane, 0.5 * (plain + edge), value)
                    term = jnp.where(cc < 3, 2.0 * EXCHANGE * INVERSE_COUNT, 0.0)
                    k2[cc, v // 2] = jnp.where(corner_lane, 0.5 * (plain - edge) + term, 0.0)
                kp[cc, v] = value

        repeat(0, 6, mend)

    for cc in range(3):
        for v in range(4):
            kp[cc, v] += INVERSE_COUNT * (lamx[...] + lam[v : v + 1, :])
    x_forward(2)

    for c in range(3):
        tiles = []
        for v in range(4):
            terms = []
            for part in range(2):
                rows = slice(64 * part, 64 * part + 64)
                total = sum(kp[PAIR[c][d], v] * spec[d, v, rows, :] for d in range(3))
                if v % 2 == 0:
                    total = total + sum(
                        k2[PAIR[c][d], v // 2] * spec[d, 4 + v // 2, rows, :] for d in range(3)
                    )
                terms.append(total)
            tiles.append(jnp.concatenate(terms, axis=0))
        out = left_product(tabx, XB, jnp.concatenate(tiles, axis=1))
        for v in range(4):
            s4[c, :, :, 8 * v : 8 * v + 8, :] = out[:, 128 * v : 128 * v + 128].reshape(2, 8, 8, 128)
        send_both(3, c, s4, r4_blocks)

    alternate = (1 - 2 * (row & 1)).astype(F32)

    def y_backward(c):
        both_arrived(3, c, r4_blocks)
        pieces = [swap_lanes([r4[c, e, pl.ds(x, 32, stride=8), :] for x in range(8)]) for e in range(2)]
        out = [[], []]
        for parity in range(2):
            value = [
                jnp.concatenate([pieces[e][2 * g + parity] for g in range(4)], axis=0) for e in range(2)
            ]
            masked = jnp.concatenate([jnp.where(low & ~lone[parity], z, 0.0) for z in value], axis=1)
            rows = wide_product(tabyb, parity, jnp.concatenate(value, axis=1))
            rows_low = wide_product(tabyb, parity, masked)
            for e in range(2):
                cols = slice(128 * e, 128 * e + 128)
                cosine, sine = rows[:128, cols], rows[128:, cols]
                cosine_low, sine_low = rows_low[:128, cols], rows_low[128:, cols]
                turned = partner(sine)
                plain = cosine + jnp.where(real, -turned, turned)
                cosine_high, sine_high = cosine - cosine_low, sine - sine_low
                base = 0.0
                if parity == 0:
                    base = value[e][0:1, :] + alternate * value[e][2:3, :]
                    cosine_high = cosine_high - base
                double = jnp.where(real, cosine_low - from_imag(sine_low), from_real(cosine_high) - sine_high)
                out[e].append(jnp.where(packed_lane, 2.0 * double + base, plain))
        for h in range(2):
            even, odd = [out[e][0] + out[e][1] if h == 0 else out[e][0] - out[e][1] for e in range(2)]
            for x, value in enumerate((even + odd, even - odd)):
                s5[pl.ds(2 * c, 2), 4 * h : 4 * h + 4, x] = value.reshape(2, 4, 16, 128)
        send_all(4, 2 * c, s5_blocks, r5, place_xy, on_xy)
        send_all(4, 2 * c + 1, s5_blocks, r5, place_xy, on_xy)

    repeat(0, 3, y_backward)

    def z_backward(n):
        arrived(4, n, r5, 16)
        tiles = [[], []]
        for parity in range(2):
            for t in range(2):
                parts = swap_lanes([r5[n, 2 * (4 * t + q) + parity] for q in range(4)])
                tiles[parity].append(jnp.concatenate(parts, axis=0))
        out = [right_product(jnp.concatenate(tiles[p], axis=1), tabz, BACKWARD + p) for p in range(2)]
        for h, value in enumerate((out[0] + out[1], out[0] - out[1])):
            s6[n, 2 * h] = value[:, 0:128]
            s6[n, 2 * h + 1] = value[:, 128:256]
        send_all(5, n, s6, r6, gz, on_z)

    repeat(0, 6, z_backward)

    def sent(e, chunks, part):
        repeat(0, chunks, lambda n: copy(e, n, part(n), part(n), by_y(lax.rem(gy + 1, 8))).wait_send())

    sent(0, 6, lambda n: r1.at[n, pl.ds(0, 3)])
    sent(1, 6, lambda n: s2.at[n, pl.ds(0, 15)])
    sent(2, 3, lambda n: s3_blocks.at[n, :, pl.ds(0, 7)])
    sent(3, 3, lambda n: s4.at[n, :, pl.ds(0, 7)])
    sent(4, 6, lambda n: s5_blocks.at[n, pl.ds(0, 15)])
    for piece in shares:
        piece.wait_send()

    @pl.when(gy == 4)
    def _():
        nyquist(top).wait_send()

    repeat(0, 6, lambda n: arrived(5, n, r6, 4))
    sent(5, 6, lambda n: s6.at[n, pl.ds(0, 3)])


def advance(m, demag, applied, pred_hbm, torque_hbm, pout, tout, sems):
    cross = lambda a, b: [
        a[1] * b[2] - a[2] * b[1],
        a[2] * b[0] - a[0] * b[2],
        a[0] * b[1] - a[1] * b[0],
    ]
    stores = []
    for s in range(4):
        planes = slice(4 * s, 4 * s + 4)
        for half in range(2):
            rows = slice(16 * half, 16 * half + 16)
            mag = [m[c, planes, rows, :] for c in range(3)]
            field = [demag[2 * c + half, s].reshape(4, 16, 128) + applied[c] for c in range(3)]
            precess = cross(mag, field)
            twist = cross(mag, precess)
            torque = [-(precess[c] + DAMPING * twist[c]) / (1.0 + DAMPING * DAMPING) for c in range(3)]
            stepped = [mag[c] + STEP * torque[c] for c in range(3)]
            length = jnp.sqrt(stepped[0] * stepped[0] + stepped[1] * stepped[1] + stepped[2] * stepped[2])
            for c in range(3):
                tout[c, planes, rows, :] = torque[c]
                pout[c, planes, rows, :] = stepped[c] / length
        stores += [
            pltpu.make_async_copy(tout.at[:, planes], torque_hbm.at[:, planes], sems.at[s, 0]),
            pltpu.make_async_copy(pout.at[:, planes], pred_hbm.at[:, planes], sems.at[s, 1]),
        ]
        stores[-2].start()
        stores[-1].start()
    for store in stores:
        store.wait()


def shards(magnetization, kernel, applied):
    zf, zb = z_tables()
    yf, yb = y_tables()
    tabz = np.stack([halves(t) for t in zf + zb])
    taby = np.stack([halves(t) for t in yf + yb])
    tabx = np.stack([left_halves(t) for t in x_tables()])
    lam, lamx = eigen_tables()
    shape = magnetization.shape
    anywhere = pl.BlockSpec(memory_space=pltpu.HBM)
    in_vmem = pl.BlockSpec(memory_space=pltpu.VMEM)
    vmem = lambda *shape, dtype=F32: pltpu.VMEM(shape, dtype)
    m, demag = pl.pallas_call(
        transform,
        out_shape=[vmem(*shape), vmem(6, 4, 64, 128)],
        in_specs=[anywhere] * 7,
        out_specs=[in_vmem, in_vmem],
        scratch_shapes=[
            vmem(6, 16, 64, 64),
            vmem(4, 2, 256, 256, dtype=BF16),
            vmem(2, 2, 256, 128, dtype=BF16),
            vmem(2, 2, 256, 128, dtype=BF16),
            vmem(3, 128, 384, dtype=BF16),
            vmem(4, 128),
            vmem(64, 128),
            vmem(6, 4, 64, 128),
            vmem(6, 2, 64, 128),
            vmem(6, 2, 64, 128),
            vmem(6, 16, 128),
            vmem(2, 6, 16, 128),
            vmem(6, 4, 4, 16, 128),
            vmem(6, 16, 16, 128),
            vmem(6, 8, 2, 16, 128),
            vmem(3, 2, 256, 128),
            vmem(3, 2, 8, 32, 128),
            vmem(3, 6, 128, 128),
            vmem(3, 2, 8, 32, 128),
            vmem(3, 2, 256, 128),
            vmem(6, 8, 2, 16, 128),
            vmem(6, 16, 16, 128),
            vmem(6, 4, 64, 128),
            pltpu.SemaphoreType.DMA((7,)),
            pltpu.SemaphoreType.DMA((6, 6)),
            pltpu.SemaphoreType.DMA((6, 6)),
            pltpu.SemaphoreType.DMA((7,)),
        ],
        compiler_params=pltpu.CompilerParams(
            collective_id=0, has_side_effects=True, vmem_limit_bytes=62 * 1024 * 1024
        ),
    )(
        magnetization, kernel, jnp.asarray(tabz), jnp.asarray(taby), jnp.asarray(tabx),
        jnp.asarray(lam), jnp.asarray(lamx),
    )
    return pl.pallas_call(
        advance,
        out_shape=[jax.ShapeDtypeStruct(shape, F32)] * 2,
        in_specs=[in_vmem, in_vmem, pl.BlockSpec(memory_space=pltpu.SMEM)],
        out_specs=[anywhere] * 2,
        scratch_shapes=[vmem(*shape), vmem(*shape), pltpu.SemaphoreType.DMA((4, 2))],
        compiler_params=pltpu.CompilerParams(vmem_limit_bytes=16 * 1024 * 1024),
    )(m, demag, applied)


def solution(mesh):
    return jax.shard_map(
        shards,
        mesh=mesh,
        in_specs=(P(None, "gx", "gy", "gz"), P(None, ("gx", "gz"), "gy", None), P()),
        out_specs=(P(None, "gx", "gy", "gz"), P(None, "gx", "gy", "gz")),
        check_vma=False,
    )
```
